32 devices in a mesh: hyp: 2 (over x), rows: 16 (over z, y, core).
Axes of the slice: x: 2, y: 2, z: 4, core: 2. Of those that a mesh axis runs over, the one named last changes fastest.
Arguments:
- offsets: float32 [2, 65536], P(None, 'rows'), may hold values from 0 to 1
- tile_cell: int32 [512], P('rows'), may hold values from 0 to 31, as said below
- probes: int32 [8, 65536], P(None, 'rows'), may hold values from 0 to 1
- target: float32 [65536], P('rows'), may hold values from -6 to 6
- lengthscale: float32 [2], P('hyp'), parts along dimension 0, may hold values from 0.5 to 1
- amplitude: float32 [2], P('hyp'), parts along dimension 0, may hold values from 0.02 to 0.08
- noise: float32 [2], P('hyp'), parts along dimension 0, may hold values from 0.1 to 0.4
Outputs:
- solutions: float32 [18, 65536], P('hyp', 'rows'), parts along dimension 0
- quadratic: float32 [18], P('hyp'), parts along dimension 0
The draws below stay inside these ranges and needn't reach their ends.
There are 2 independent parts, one for each index of `hyp`. The reference program is written for one: setup_inputs(seed, part) draws one part's arguments, and reference() takes and returns one part's arrays. A program takes and returns all parts, laid end to end along the dimension named above; an argument that names none is the same for every part. Nothing has to cross between parts.
Inputs may be any that keep to these rules, and one draw needn't show every extreme that they name: `tile_cell`: each aligned block of 32 entries (one device's tiles) is a permutation of 0 to 31.
All inputs are finite; a program needn't handle non-finite values.
Results may differ from the reference program's by a relative error of at most 0.0003.
Values sent between devices are 32-bit elements; how exact they have to be, the bound alone decides.
A program may use at most 64 MiB of HBM per device.

```python
import math
import jax
import jax.numpy as jnp
from jax import lax

TILE = 128
GX = 16
PROBES = 8
ITERS = 3
RHS = 9
TPD = 32
NTR = 32
NTILES = 512
NPTS = 65536


def draw_tile_cell(key, part):
    scores = jax.random.randint(jax.random.fold_in(key, 17), (NTILES // TPD, TPD), 0, 1 << 30)
    placing = jnp.argsort(scores, axis=1, stable=True)
    return placing.reshape(NTILES).astype(jnp.int32)


def set_ends(drawn, key, least, top_value):
    place = [jax.random.randint(jax.random.fold_in(key, axis), (), 0, length) for axis, length in enumerate(drawn.shape)]
    main_axis = drawn.shape.index(max(drawn.shape))
    neighbour = place[:main_axis] + [(place[main_axis] + 1) % drawn.shape[main_axis]] + place[main_axis + 1:]
    return drawn.at[tuple(place)].set(least).at[tuple(neighbour)].set(top_value)


def block_scale(key, dims, shards, low, largest):
    def one(dim, shards_of):
        draws = jax.random.uniform(jax.random.fold_in(jax.random.fold_in(key, 6), dim), (shards_of,), jnp.float32, low / len(shards), largest / len(shards))
        return jnp.repeat(jnp.exp(draws), dims[dim] // shards_of).reshape((-1,) + (1,) * (len(dims) - dim - 1))

    factor_of = one(*shards[0])
    for cut in shards[1:]:
        factor_of = factor_of * one(*cut)
    return factor_of


def scatter_about(key, extent, scale, reach, shards=(), kind=jnp.bfloat16):
    array = scale * jax.random.normal(key, extent, jnp.float32)
    if shards:
        array = array * block_scale(key, extent, shards, -0.22, 0.18)
    return jnp.clip(array, -reach, reach).astype(kind)


def setup_inputs(seed: int = 0, part: int = 0) -> dict:
    streams_of = jax.random.split(jax.random.key(seed), 8)
    part_splits = jax.random.split(jax.random.fold_in(streams_of[7], part), 8)
    offsets = jnp.clip(1.0 * jax.random.uniform(streams_of[0], (2, NPTS), jnp.float32) ** block_scale(streams_of[0], (2, NPTS), ((1, 16),), -0.2, 0.2), 0.0, 1.0)
    tile_cell = draw_tile_cell(jax.random.fold_in(streams_of[7], 71), part)
    probes = set_ends(jax.random.randint(streams_of[2], (PROBES, NPTS), 0, 2), jax.random.fold_in(streams_of[2], 1), 0, 1).astype(jnp.int32)
    target = scatter_about(streams_of[3], (NPTS,), 1.0, 6.0, ((0, 16),), jnp.float32)
    lengthscale = jnp.clip(jnp.exp(jax.random.uniform(part_splits[4], (1,), jnp.float32, math.log(0.5), math.log(1.0))), 0.5, 1.0)
    amplitude = jnp.clip(jnp.exp(jax.random.uniform(part_splits[5], (1,), jnp.float32, math.log(0.02), math.log(0.08))), 0.02, 0.08)
    noise = jnp.clip(jnp.exp(jax.random.uniform(part_splits[6], (1,), jnp.float32, math.log(0.1), math.log(0.4))), 0.1, 0.4)
    return {"offsets": offsets, "tile_cell": tile_cell, "probes": probes, "target": target, "lengthscale": lengthscale, "amplitude": amplitude, "noise": noise}


def wendland(distance):
    closeness = jnp.maximum(1.0 - distance, 0.0)
    return closeness ** 4 * (4.0 * distance + 1.0)

def kernel_sum(vectors, padded_vectors, coords, padded_coords, inverse_length, amplitude, noise):
    row_count = vectors.shape[1]
    col_count = vectors.shape[2]
    total = noise * vectors
    for row_shift in (-1, 0, 1):
        for col_shift in (-1, 0, 1):
            other = padded_coords[:, 1 + row_shift:1 + row_shift + row_count, 1 + col_shift:1 + col_shift + col_count, :]
            values = padded_vectors[:, 1 + row_shift:1 + row_shift + row_count, 1 + col_shift:1 + col_shift + col_count, :]
            delta_rows = coords[0][..., :, None] - other[0][..., None, :]
            delta_cols = coords[1][..., :, None] - other[1][..., None, :]
            distance = jnp.sqrt(delta_rows * delta_rows + delta_cols * delta_cols) * inverse_length
            weights = amplitude * wendland(distance)
            total = total + jnp.einsum('rabj,abij->rabi', values, weights, precision=lax.Precision.HIGHEST)
    return total

def to_grid(stored, order):
    lead = stored.shape[0]
    tiles = stored.reshape(lead, NTILES, TILE)[:, order]
    return tiles.reshape(lead, NTR, GX, TILE)

def reference(offsets, tile_cell, probes, target, lengthscale, amplitude, noise):
    device_base = jnp.arange(NTILES, dtype=jnp.int32) // TPD * TPD
    cell = (tile_cell + device_base).astype(jnp.int32)
    order = jnp.argsort(cell).astype(jnp.int32)
    grid_offsets = to_grid(offsets, order)
    row_place = jnp.arange(NTR, dtype=jnp.float32)[:, None, None]
    col_place = jnp.arange(GX, dtype=jnp.float32)[None, :, None]
    coords = jnp.stack([grid_offsets[0] + row_place, grid_offsets[1] + col_place])
    padded_coords = jnp.pad(coords, ((0, 0), (1, 1), (1, 1), (0, 0)))
    signs = 2.0 * probes.astype(jnp.float32) - 1.0
    right_sides = to_grid(jnp.concatenate([signs, target[None, :]], axis=0), order)
    inverse_length = 1.0 / lengthscale[0]

    def operate(vectors):
        padded = jnp.pad(vectors, ((0, 0), (1, 1), (1, 1), (0, 0)))
        return kernel_sum(vectors, padded, coords, padded_coords, inverse_length, amplitude[0], noise[0])

    def widen(scalars):
        return scalars[:, None, None, None]
    iterate = jnp.zeros_like(right_sides)
    residual = right_sides
    direction = right_sides
    norm_now = lax.optimization_barrier(jnp.sum(residual * residual, axis=(1, 2, 3)))
    for iteration in range(ITERS):
        image = operate(direction)
        alpha = norm_now / lax.optimization_barrier(jnp.sum(direction * image, axis=(1, 2, 3)))
        iterate = iterate + widen(alpha) * direction
        residual = residual - widen(alpha) * image
        if iteration + 1 < ITERS:
            norm_next = lax.optimization_barrier(jnp.sum(residual * residual, axis=(1, 2, 3)))
            direction = residual + widen(norm_next / norm_now) * direction
            norm_now = norm_next
    quadratic = lax.optimization_barrier(jnp.sum(right_sides * iterate, axis=(1, 2, 3))) / NPTS
    solutions = iterate.reshape(RHS, NTILES, TILE)[:, cell].reshape(RHS, NPTS)
    return (solutions, quadratic)
```

```python
import functools

import jax
import jax.numpy as jnp
from jax import lax
from jax.experimental import pallas as pl
from jax.experimental.pallas import tpu as pltpu
from jax.sharding import PartitionSpec as P

TILE = 128
GX = 16
RHS = 9
PAD = 16
FAR = 1.0e3
SNAP = 12.0
NUDGE = 2.0**-21
MESH = pl.DeviceIdType.MESH
F32 = jnp.float32
BF16 = jnp.bfloat16


def snap(value):
    return (value + SNAP) - SNAP


def kernel(
    n, rows, points,
    cell, length, amp_ref, noise_ref, off_in, probes_in, target_in,
    x_ref, q_ref,
    off, probes, target, raw, vec, last, place, snapped, hvec, hlast, hplace,
    vx, vh, whi, wlo, ohi, olo, even, odd, acc, mom, gathered,
    powers, load_sem, halo_send, halo_recv, mom_send, mom_recv,
):
    tiles = rows * GX
    wide = rows * TILE
    me = lax.axis_index("rows")
    has = (me > 0, me < n - 1)
    amp = amp_ref[0]
    shift = amp + noise_ref[0]

    barrier = pltpu.get_barrier_semaphore()

    def greet(k, carry):
        pl.semaphore_signal(
            barrier, inc=1, device_id={"rows": lax.rem(me + k, n)}, device_id_type=MESH
        )
        return carry

    lax.fori_loop(1, n, greet, 0)
    loads = [
        pltpu.make_async_copy(source, held, load_sem.at[i])
        for i, (source, held) in enumerate(
            ((off_in, off), (probes_in, probes), (target_in, target))
        )
    ]
    for load in loads:
        load.start()

    for s in range(tiles):
        powers[s] = jnp.int32((1 << s) - ((1 << 32) if s == 31 else 0))
    words = [jnp.int32(0)] * (tiles - 1).bit_length()
    for s in range(tiles):
        bit = powers[cell[s]]
        words = [w | bit if (s >> b) & 1 else w for b, w in enumerate(words)]
    order = []
    for g in range(tiles):
        place_of = jnp.int32(0)
        for b, w in enumerate(words):
            one = lax.shift_right_logical(w, jnp.int32(g)) & 1
            place_of = place_of | lax.shift_left(one, jnp.int32(b))
        order.append(place_of)

    inverse = 1.0 / jnp.full((1, TILE), length[0], F32)
    step = snap(inverse)

    def split(value):
        high = value.astype(BF16)
        return jnp.concatenate([high, (value - high.astype(F32)).astype(BF16)], axis=0)

    for edge in (0, GX + 1):
        for par in range(2):
            vx[par, edge] = jnp.zeros((2 * PAD, wide), BF16)
        for side in range(2):
            vh[side, edge] = jnp.zeros((2 * PAD, TILE), BF16)
    for held in (whi, wlo):
        held[0, 0] = jnp.zeros((wide, wide), BF16)
        held[GX - 1, 2] = jnp.zeros((wide, wide), BF16)

    for load in loads:
        load.wait()

    for g in range(tiles):
        at = slice(g * TILE, (g + 1) * TILE)
        raw[g] = jnp.concatenate(
            [
                2.0 * probes[:, at].astype(F32) - 1.0,
                target[:, at],
                off[:, at],
                jnp.zeros((PAD - RHS - 2, TILE), F32),
            ],
            axis=0,
        )
    kept = lax.broadcasted_iota(jnp.int32, (PAD, TILE), 0) < RHS
    for c in range(GX):
        for a in range(rows):
            value = raw[order[a * GX + c]]
            where = value[RHS : RHS + 2]
            value = jnp.where(kept, value, 0.0)
            vec[0, c, a] = value
            last[0, a, c] = value[RHS - 1 : RHS]
            place[a, c] = where
            snapped[c, a] = snap(where * inverse)
            vx[0, c + 1, :, a * TILE : (a + 1) * TILE] = split(value)

    def copies(k, side):
        row = 0 if side == 0 else rows - 1
        pairs = [
            (vec.at[k, :, row, 0 : RHS - 1, :], hvec.at[k, 1 - side]),
            (last.at[k, row], hlast.at[k, 1 - side]),
        ]
        if k == 0:
            pairs.append((place.at[row], hplace.at[1 - side]))
        return [
            pltpu.make_async_remote_copy(
                src_ref=source,
                dst_ref=target_ref,
                send_sem=halo_send.at[k, side, i],
                recv_sem=halo_recv.at[k, 1 - side, i],
                device_id={"rows": me - 1 if side == 0 else me + 1},
                device_id_type=MESH,
            )
            for i, (source, target_ref) in enumerate(pairs)
        ]

    def sends(k):
        return (0, 1) if k < 2 else (0,)

    def send_halo(k):
        for side in sends(k):
            @pl.when(has[side])
            def _(side=side):
                for copy in copies(k, side):
                    copy.start()

    def receive_halo(k):
        for side in sends(k):
            @pl.when(has[1 - side])
            def _(side=side):
                for i, dst in enumerate((hvec.at[k, 1 - side], hlast.at[k, 1 - side], hplace.at[1 - side])):
                    if i < 2 or k == 0:
                        pltpu.make_async_remote_copy(
                            src_ref=dst,
                            dst_ref=dst,
                            send_sem=halo_send.at[k, side, i],
                            recv_sem=halo_recv.at[k, 1 - side, i],
                            device_id={"rows": me + 1 if side == 0 else me - 1},
                            device_id_type=MESH,
                        ).wait_recv()

            @pl.when(jnp.logical_not(has[1 - side]))
            def _(side=side):
                hvec[k, 1 - side] = jnp.zeros(hvec.shape[2:], F32)
                hlast[k, 1 - side] = jnp.zeros(hlast.shape[2:], F32)
                if k == 0:
                    hplace[1 - side] = jnp.full(hplace.shape[1:], FAR, F32)

            for c in range(GX):
                vh[1 - side, c + 1] = split(
                    jnp.concatenate(
                        [hvec[k, 1 - side, c], hlast[k, 1 - side, c], jnp.zeros((PAD - RHS, TILE), F32)],
                        axis=0,
                    )
                )

    def spread(held, where):
        for axis in range(2):
            held[axis] = jnp.broadcast_to(where[axis : axis + 1], (TILE, TILE)).T

    def weights(held, where, down, right):
        tx = where[0:1] + (down * step + NUDGE)
        ty = where[1:2] + right * step
        high, low = [], []
        size = 64
        for part in range(TILE // size):
            at = slice(part * size, (part + 1) * size)
            dx = held[0, at, :] - tx
            dy = held[1, at, :] - ty
            square = dx * dx + dy * dy
            close = jnp.maximum(1.0 - square * lax.rsqrt(square), 0.0)
            twice = close * close
            w = twice * twice * (1.25 - close)
            top = w.astype(BF16)
            high.append(top)
            low.append((w - top.astype(F32)).astype(BF16))
        return jnp.concatenate(high, axis=0), jnp.concatenate(low, axis=0)

    def put(c, j, source, to, pair):
        down = slice(source * TILE, (source + 1) * TILE)
        right = slice(to * TILE, (to + 1) * TILE)
        whi[c, j, down, right] = pair[0]
        wlo[c, j, down, right] = pair[1]

    def column(c, held, fresh, more=True):
        if more:
            for a in range(rows):
                spread(fresh.at[a], snapped[c + 1, a])
        for a in range(rows):
            for b in range(a, rows):
                pair = weights(held.at[a], snapped[c, b], b - a, 0)
                put(c, 1, a, b, pair)
                if b > a:
                    put(c, 1, b, a, tuple(p.T for p in pair))
        if more:
            for a in range(rows):
                for b in range(rows):
                    pair = weights(held.at[a], snapped[c + 1, b], b - a, 1)
                    put(c + 1, 0, a, b, pair)
                    put(c, 2, b, a, tuple(p.T for p in pair))

    def two(i, carry):
        column(2 * i, even, odd)
        column(2 * i + 1, odd, even)
        return carry

    for a in range(rows):
        spread(even.at[a], snapped[0, a])
    half = GX // 2 - 1
    lax.fori_loop(0, half - 3, two, 0)
    pl.semaphore_wait(barrier, n - 1)
    send_halo(0)
    lax.fori_loop(half - 3, half, two, 0)
    column(GX - 2, even, odd)
    column(GX - 1, odd, even, more=False)

    def apply(v, high, low):
        r = jnp.dot(v, high, preferred_element_type=F32)
        s = jnp.dot(v[:PAD], low, preferred_element_type=F32)
        return r[:PAD] + r[PAD:] + s

    def inner(par, count):
        def run(c, carry):
            v = [vx[par, c + j] for j in range(count)]
            if count < 3:
                v[1] = v[1] * BF16(0.5)
            high, low = (
                jnp.concatenate([held[c, j] for j in range(count)], axis=0)
                for held in (whi, wlo)
            )
            acc[c] = apply(jnp.concatenate(v, axis=1), high, low)
            return carry

        lax.fori_loop(0, GX, run, 0, unroll=8)

    def outer_weights(p, carry):
        for side in range(2):
            row = 0 if side == 0 else rows - 1
            down = 1 if side == 0 else -1
            for held in (ohi, olo):
                held[side, p + 1, 0, 3 * TILE :] = jnp.zeros((TILE, TILE), BF16)
                held[side, p + 1, 1, :TILE] = jnp.zeros((TILE, TILE), BF16)
            for t in range(2):
                c = 2 * p + t
                fresh = (even, odd)[side].at[t]
                spread(fresh, snap(hplace[side, c] * inverse))
                for move in (-1, 0, 1):
                    spot = t + move
                    to, slot = p + 1 + spot // 2, spot % 2
                    source = t + 1 - 2 * (spot // 2)
                    near = jnp.clip(c + move, 0, GX - 1)
                    high, low = weights(fresh, snapped[near, row], down, move)
                    down_at = slice(source * TILE, (source + 1) * TILE)
                    ohi[side, to, slot, down_at] = high
                    olo[side, to, slot, down_at] = low
        return carry

    def outer(k, par):
        def run(p, carry):
            first, cross, square = carry
            edges = {}
            for side in (0, 1) if k < 2 else (1,):
                v = jnp.concatenate([vh[side, 2 * p + j] for j in range(4)], axis=1)
                high, low = (
                    jnp.concatenate([held[side, p + 1, t] for t in range(2)], axis=1)
                    for held in (ohi, olo)
                )
                edges[side] = apply(v, high, low)
            for t in range(2):
                c = 2 * p + t
                for a in range(rows):
                    total = acc[c, :, a * TILE : (a + 1) * TILE]
                    for side, row in ((0, 0), (1, rows - 1)):
                        if a == row and side in edges:
                            total = total + edges[side][:, t * TILE : (t + 1) * TILE]
                    now = vec[k, c, a]
                    if k < 2:
                        later = (4.0 * amp) * total - amp * now
                        if k == 0:
                            first = first + now * now
                        cross = cross + now * later
                        square = square + later * later
                        vec[k + 1, c, a] = later
                        last[k + 1, a, c] = later[RHS - 1 : RHS]
                        vx[1 - par, c + 1, :, a * TILE : (a + 1) * TILE] = split(later)
                    else:
                        cross = cross + now * total
            return first, cross, square

        blank = jnp.zeros((PAD, TILE), F32)
        return lax.fori_loop(0, GX // 2, run, (blank, blank, blank), unroll=8)

    moments = []
    for k in range(3):
        par = k % 2
        inner(par, 3 if k < 2 else 2)
        receive_halo(k)
        if k == 0:
            lax.fori_loop(0, GX // 2, outer_weights, 0)
            for side in range(2):
                for held in (ohi, olo):
                    held[side, 1, 0, :TILE] = jnp.zeros((TILE, TILE), BF16)
                    held[side, GX // 2, 1, 3 * TILE :] = jnp.zeros((TILE, TILE), BF16)
        first, cross, square = outer(k, par)
        if k == 0:
            moments.append(first)
        if k < 2:
            moments += [cross, square]
            send_halo(k + 1)
        else:
            moments.append((8.0 * amp) * cross - amp * moments[4])

    lane = lax.broadcasted_iota(jnp.int32, (RHS - 1, TILE), 1)
    packed = jnp.zeros((RHS - 1, TILE), F32)
    for i, part in enumerate(moments):
        total = jnp.sum(part, axis=1, keepdims=True)
        packed = jnp.where(lane == i, total[: RHS - 1], packed)
        packed = jnp.where(lane == i + len(moments), total[RHS - 1 : RHS], packed)
    mom[...] = packed
    gathered[me] = packed

    def mom_copy(k):
        peer = lax.rem(me + k, n)
        return pltpu.make_async_remote_copy(
            src_ref=mom,
            dst_ref=gathered.at[me],
            send_sem=mom_send.at[peer],
            recv_sem=mom_recv.at[me],
            device_id={"rows": peer},
            device_id_type=MESH,
        )

    def mom_start(k, carry):
        mom_copy(k).start()
        return carry

    lax.fori_loop(1, n, mom_start, 0)

    def mom_wait(k, carry):
        peer = lax.rem(me + k, n)
        pltpu.make_async_remote_copy(
            src_ref=mom,
            dst_ref=gathered.at[peer],
            send_sem=mom_send.at[peer],
            recv_sem=mom_recv.at[peer],
            device_id={"rows": peer},
            device_id_type=MESH,
        ).wait()
        return carry

    lax.fori_loop(1, n, mom_wait, 0)
    total = lax.fori_loop(0, n, lambda j, t: t + gathered[j], jnp.zeros((RHS - 1, TILE), F32))

    m = [
        jnp.concatenate([total[:, i : i + 1], total[:, i + 6 : i + 7]], axis=0)
        for i in range(6)
    ]
    a00, a01, a02 = (m[i + 1] + shift * m[i] for i in range(3))
    a11, a12 = (m[i + 1] + shift * m[i] for i in range(2, 4))
    a22 = m[5] + shift * m[4]
    l1 = a01 / a00
    l2 = a02 / a00
    b11 = a11 - l1 * a01
    b12 = a12 - l1 * a02
    b22 = a22 - l2 * a02
    g1 = m[1] - l1 * m[0]
    g2 = m[2] - l2 * m[0]
    fine1 = b11 > 1.0e-6 * a11
    safe1 = jnp.where(fine1, b11, 1.0)
    l3 = b12 / safe1
    d22 = b22 - l3 * b12
    fine2 = jnp.logical_and(fine1, d22 > 1.0e-6 * a22)
    c2 = jnp.where(fine2, (g2 - l3 * g1) / jnp.where(fine2, d22, 1.0), 0.0)
    c1 = jnp.where(fine1, (g1 - b12 * c2) / safe1, 0.0)
    c0 = (m[0] - a01 * c1 - a02 * c2) / a00
    values = (c0 * m[0] + c1 * m[1] + c2 * m[2]) / points
    flat = lax.broadcasted_iota(jnp.int32, (PAD, TILE), 1)
    sublane = lax.broadcasted_iota(jnp.int32, (PAD, TILE), 0)
    turned = jnp.sum(jnp.where(flat == sublane, values, 0.0), axis=0, keepdims=True)
    q_ref[...] = turned[:, :RHS]

    c0, c1, c2 = (jnp.broadcast_to(c, (PAD, TILE)) for c in (c0, c1, c2))
    for s in range(tiles):
        spot = cell[s]
        a, c = spot // GX, spot % GX
        found = c0 * vec[0, c, a] + c1 * vec[1, c, a] + c2 * vec[2, c, a]
        x_ref[:, s * TILE : (s + 1) * TILE] = found[:RHS]

    for k in range(3):
        for side in sends(k):
            @pl.when(has[side])
            def _(k=k, side=side):
                for copy in copies(k, side):
                    copy.wait_send()


def shards(n, offsets, tile_cell, probes, target, lengthscale, amplitude, noise):
    tiles = tile_cell.shape[0]
    rows = tiles // GX
    local = tiles * TILE
    wide = rows * TILE
    smem = pl.BlockSpec(memory_space=pltpu.SMEM)
    vmem = pl.BlockSpec(memory_space=pltpu.VMEM)
    solutions, quadratic = pl.pallas_call(
        functools.partial(kernel, n, rows, float(local * n)),
        out_shape=(
            jax.ShapeDtypeStruct((RHS, local), F32),
            jax.ShapeDtypeStruct((1, RHS), F32),
        ),
        in_specs=[smem] * 4 + [pl.BlockSpec(memory_space=pl.ANY)] * 3,
        out_specs=(vmem, vmem),
        scratch_shapes=[
            pltpu.VMEM((2, local), F32),
            pltpu.VMEM((RHS - 1, local), jnp.int32),
            pltpu.VMEM((1, local), F32),
            pltpu.VMEM((tiles, PAD, TILE), F32),
            pltpu.VMEM((3, GX, rows, PAD, TILE), F32),
            pltpu.VMEM((3, rows, GX, 1, TILE), F32),
            pltpu.VMEM((rows, GX, 2, TILE), F32),
            pltpu.VMEM((GX, rows, 2, TILE), F32),
            pltpu.VMEM((3, 2, GX, RHS - 1, TILE), F32),
            pltpu.VMEM((3, 2, GX, 1, TILE), F32),
            pltpu.VMEM((2, GX, 2, TILE), F32),
            pltpu.VMEM((2, GX + 2, 2 * PAD, wide), BF16),
            pltpu.VMEM((2, GX + 2, 2 * PAD, TILE), BF16),
            pltpu.VMEM((GX, 3, wide, wide), BF16),
            pltpu.VMEM((GX, 3, wide, wide), BF16),
            pltpu.VMEM((2, GX // 2 + 2, 2, 4 * TILE, TILE), BF16),
            pltpu.VMEM((2, GX // 2 + 2, 2, 4 * TILE, TILE), BF16),
            pltpu.VMEM((rows, 2, TILE, TILE), F32),
            pltpu.VMEM((rows, 2, TILE, TILE), F32),
            pltpu.VMEM((GX, PAD, wide), F32),
            pltpu.VMEM((RHS - 1, TILE), F32),
            pltpu.VMEM((n, RHS - 1, TILE), F32),
            pltpu.SMEM((tiles,), jnp.int32),
            pltpu.SemaphoreType.DMA((3,)),
            pltpu.SemaphoreType.DMA((3, 2, 3)),
            pltpu.SemaphoreType.DMA((3, 2, 3)),
            pltpu.SemaphoreType.DMA((n,)),
            pltpu.SemaphoreType.DMA((n,)),
        ],
        compiler_params=pltpu.CompilerParams(
            collective_id=0, has_side_effects=True, vmem_limit_bytes=52 * 1024 * 1024
        ),
        name="solve",
    )(tile_cell, lengthscale, amplitude, noise, offsets, probes, target[None, :])
    return solutions, quadratic.reshape(RHS)


def solution(mesh):
    return jax.shard_map(
        functools.partial(shards, mesh.shape["rows"]),
        mesh=mesh,
        in_specs=(
            P(None, "rows"),
            P("rows"),
            P(None, "rows"),
            P("rows"),
            P("hyp"),
            P("hyp"),
            P("hyp"),
        ),
        out_specs=(P("hyp", "rows"), P("hyp")),
        check_vma=False,
    )
```

```python
import functools

import jax
import jax.numpy as jnp
from jax import lax
from jax.experimental import pallas as pl
from jax.experimental.pallas import tpu as pltpu
from jax.sharding import PartitionSpec as P

TILE = 128
GX = 16
RHS = 9
PAD = 16
FAR = 1.0e3
SCALE = 8.0
SNAP = 12.0 * SCALE
NUDGE = SCALE * 2.0**-21
GAIN = 4.0 / SCALE**5
MESH = pl.DeviceIdType.MESH
F32 = jnp.float32
BF16 = jnp.bfloat16
F8 = jnp.float8_e4m3fn


def snap(value):
    return (value + SNAP) - SNAP


def kernel(
    n, rows, points,
    cell_in, off_in, probes_in, target_in, length, amp_ref, noise_ref,
    x_ref, q_ref,
    cell, off, probes, target, raw, vec, last, place, snapped, hvec, hlast, hplace,
    vx, vh, whi, wlo, ohi, olo, even, odd, acc, mom, gathered,
    powers, load_sem, halo_send, halo_recv, mom_send, mom_recv,
):
    tiles = rows * GX
    wide = rows * TILE
    me = lax.axis_index("rows")
    has = (me > 0, me < n - 1)

    barrier = pltpu.get_barrier_semaphore()

    def greet(k, carry):
        pl.semaphore_signal(
            barrier, inc=1, device_id={"rows": lax.rem(me + k, n)}, device_id_type=MESH
        )
        return carry

    loads = [
        pltpu.make_async_copy(source, held, load_sem.at[i])
        for i, (source, held) in enumerate(
            (
                (cell_in, cell), (off_in, off), (probes_in, probes), (target_in, target),
            )
        )
    ]
    for load in loads:
        load.start()
    lax.fori_loop(1, n, greet, 0)
    loads[0].wait()
    amp = amp_ref[0]
    shift = amp + noise_ref[0]

    for s in range(tiles):
        powers[s] = jnp.int32((1 << s) - ((1 << 32) if s == 31 else 0))
    words = [jnp.int32(0)] * (tiles - 1).bit_length()
    for s in range(tiles):
        bit = powers[cell[s]]
        words = [w | bit if (s >> b) & 1 else w for b, w in enumerate(words)]
    order = []
    for g in range(tiles):
        place_of = jnp.int32(0)
        for b, w in enumerate(words):
            one = lax.shift_right_logical(w, jnp.int32(g)) & 1
            place_of = place_of | lax.shift_left(one, jnp.int32(b))
        order.append(place_of)

    inverse = SCALE / jnp.full((1, TILE), length[0], F32)
    step = snap(inverse)

    def split(value):
        high = value.astype(BF16)
        return jnp.concatenate([high, (value - high.astype(F32)).astype(BF16)], axis=0)

    for edge in (0, GX + 1):
        for par in range(2):
            vx[par, edge] = jnp.zeros((2 * PAD, wide), BF16)
        for side in range(2):
            vh[side, edge] = jnp.zeros((2 * PAD, TILE), BF16)
    for held in (whi, wlo):
        held[0, 0] = jnp.zeros((wide, wide), held.dtype)
        held[GX - 1, 2] = jnp.zeros((wide, wide), held.dtype)

    for load in loads[1:]:
        load.wait()

    for g in range(tiles):
        at = slice(g * TILE, (g + 1) * TILE)
        raw[g] = jnp.concatenate(
            [
                2.0 * probes[:, at].astype(F32) - 1.0,
                target[:, at],
                off[:, at],
                jnp.zeros((PAD - RHS - 2, TILE), F32),
            ],
            axis=0,
        )
    kept = lax.broadcasted_iota(jnp.int32, (PAD, TILE), 0) < RHS
    for c in range(GX):
        for a in range(rows):
            value = raw[order[a * GX + c]]
            where = value[RHS : RHS + 2]
            value = jnp.where(kept, value, 0.0)
            vec[0, c, a] = value
            last[0, a, c] = value[RHS - 1 : RHS]
            place[a, c] = where
            snapped[c, a] = snap(where * inverse)
            vx[0, c + 1, :, a * TILE : (a + 1) * TILE] = split(value)

    def copies(k, side):
        row = 0 if side == 0 else rows - 1
        pairs = [
            (vec.at[k, :, row, 0 : RHS - 1, :], hvec.at[k, 1 - side]),
            (last.at[k, row], hlast.at[k, 1 - side]),
        ]
        if k == 0:
            pairs.append((place.at[row], hplace.at[1 - side]))
        return [
            pltpu.make_async_remote_copy(
                src_ref=source,
                dst_ref=target_ref,
                send_sem=halo_send.at[k, side, i],
                recv_sem=halo_recv.at[k, 1 - side, i],
                device_id={"rows": me - 1 if side == 0 else me + 1},
                device_id_type=MESH,
            )
            for i, (source, target_ref) in enumerate(pairs)
        ]

    def sends(k):
        return (0, 1) if k < 2 else (0,)

    def send_halo(k):
        for side in sends(k):
            @pl.when(has[side])
            def _(side=side):
                for copy in copies(k, side):
                    copy.start()

    def receive_halo(k):
        for side in sends(k):
            @pl.when(has[1 - side])
            def _(side=side):
                for i, dst in enumerate((hvec.at[k, 1 - side], hlast.at[k, 1 - side], hplace.at[1 - side])):
                    if i < 2 or k == 0:
                        pltpu.make_async_remote_copy(
                            src_ref=dst,
                            dst_ref=dst,
                            send_sem=halo_send.at[k, side, i],
                            recv_sem=halo_recv.at[k, 1 - side, i],
                            device_id={"rows": me + 1 if side == 0 else me - 1},
                            device_id_type=MESH,
                        ).wait_recv()

            @pl.when(jnp.logical_not(has[1 - side]))
            def _(side=side):
                hvec[k, 1 - side] = jnp.zeros(hvec.shape[2:], F32)
                hlast[k, 1 - side] = jnp.zeros(hlast.shape[2:], F32)
                if k == 0:
                    hplace[1 - side] = jnp.full(hplace.shape[1:], FAR, F32)

            for c in range(GX):
                vh[1 - side, c + 1] = split(
                    jnp.concatenate(
                        [hvec[k, 1 - side, c], hlast[k, 1 - side, c], jnp.zeros((PAD - RHS, TILE), F32)],
                        axis=0,
                    )
                )

    def spread(held, where):
        for axis in range(2):
            held[axis] = jnp.broadcast_to(where[axis : axis + 1], (TILE, TILE)).T

    def weights(held, where, down, right):
        tx = where[0:1] + (down * step + NUDGE)
        ty = where[1:2] + right * step
        high, low = [], []
        size = 64
        for part in range(TILE // size):
            at = slice(part * size, (part + 1) * size)
            dx = held[0, at, :] - tx
            dy = held[1, at, :] - ty
            square = dx * dx + dy * dy
            close = jnp.maximum(SCALE - square * lax.rsqrt(square), 0.0)
            twice = close * close
            w = twice * twice * (1.25 * SCALE - close)
            top = w.astype(BF16)
            high.append(top)
            low.append((w - top.astype(F32)).astype(F8))
        return jnp.concatenate(high, axis=0), jnp.concatenate(low, axis=0)

    def put(c, j, source, to, pair):
        down = slice(source * TILE, (source + 1) * TILE)
        right = slice(to * TILE, (to + 1) * TILE)
        whi[c, j, down, right] = pair[0]
        wlo[c, j, down, right] = pair[1]

    def column(c, held, fresh, more=True):
        if more:
            for a in range(rows):
                spread(fresh.at[a], snapped[c + 1, a])
        for a in range(rows):
            for b in range(a, rows):
                pair = weights(held.at[a], snapped[c, b], b - a, 0)
                put(c, 1, a, b, pair)
                if b > a:
                    put(c, 1, b, a, tuple(p.T for p in pair))
        if more:
            for a in range(rows):
                for b in range(rows):
                    pair = weights(held.at[a], snapped[c + 1, b], b - a, 1)
                    put(c + 1, 0, a, b, pair)
                    put(c, 2, b, a, tuple(p.T for p in pair))

    def two(i, carry):
        column(2 * i, even, odd)
        column(2 * i + 1, odd, even)
        return carry

    for a in range(rows):
        spread(even.at[a], snapped[0, a])
    half = GX // 2 - 1
    lax.fori_loop(0, half - 5, two, 0)
    pl.semaphore_wait(barrier, n - 1)
    send_halo(0)
    lax.fori_loop(half - 5, half, two, 0)
    column(GX - 2, even, odd)
    column(GX - 1, odd, even, more=False)

    def apply(v, high, low):
        r = jnp.dot(v, high, preferred_element_type=F32)
        s = jnp.dot(v[:PAD], low, preferred_element_type=F32)
        return r[:PAD] + r[PAD:] + s

    def inner_run(par, count):
        def run(c, carry):
            v = [vx[par, c + j] for j in range(count)]
            if count < 3:
                v[1] = v[1] * BF16(0.5)
            high, low = (
                jnp.concatenate([held[c, j] for j in range(count)], axis=0)
                for held in (whi, wlo)
            )
            acc[c] = apply(jnp.concatenate(v, axis=1), high, low)
            return carry

        return run

    def inner(par, count):
        lax.fori_loop(0, GX, inner_run(par, count), 0, unroll=16)

    def outer_weights(p, carry):
        inner_run(0, 3)(2 * p, 0)
        inner_run(0, 3)(2 * p + 1, 0)
        for side in range(2):
            row = 0 if side == 0 else rows - 1
            down = 1 if side == 0 else -1
            for held in (ohi, olo):
                held[side, p + 1, 0, 3 * TILE :] = jnp.zeros((TILE, TILE), held.dtype)
                held[side, p + 1, 1, :TILE] = jnp.zeros((TILE, TILE), held.dtype)
            for t in range(2):
                c = 2 * p + t
                fresh = (even, odd)[side].at[t]
                spread(fresh, snap(hplace[side, c] * inverse))
                for move in (-1, 0, 1):
                    spot = t + move
                    to, slot = p + 1 + spot // 2, spot % 2
                    source = t + 1 - 2 * (spot // 2)
                    near = jnp.clip(c + move, 0, GX - 1)
                    high, low = weights(fresh, snapped[near, row], down, move)
                    down_at = slice(source * TILE, (source + 1) * TILE)
                    ohi[side, to, slot, down_at] = high
                    olo[side, to, slot, down_at] = low
        return carry

    def outer(k, par):
        def run(p, carry):
            first, cross, square = carry
            edges = {}
            for side in (0, 1) if k < 2 else (1,):
                v = jnp.concatenate([vh[side, 2 * p + j] for j in range(4)], axis=1)
                high, low = (
                    jnp.concatenate([held[side, p + 1, t] for t in range(2)], axis=1)
                    for held in (ohi, olo)
                )
                edges[side] = apply(v, high, low)
            for t in range(2):
                c = 2 * p + t
                for a in range(rows):
                    total = acc[c, :, a * TILE : (a + 1) * TILE]
                    for side, row in ((0, 0), (1, rows - 1)):
                        if a == row and side in edges:
                            total = total + edges[side][:, t * TILE : (t + 1) * TILE]
                    now = vec[k, c, a]
                    if k < 2:
                        later = (GAIN * amp) * total - amp * now
                        if k == 0:
                            first = first + now * now
                        cross = cross + now * later
                        square = square + later * later
                        vec[k + 1, c, a] = later
                        last[k + 1, a, c] = later[RHS - 1 : RHS]
                        vx[1 - par, c + 1, :, a * TILE : (a + 1) * TILE] = split(later)
                    else:
                        cross = cross + now * total
            return first, cross, square

        blank = jnp.zeros((PAD, TILE), F32)
        return lax.fori_loop(0, GX // 2, run, (blank, blank, blank), unroll=8)

    moments = []
    for k in range(3):
        par = k % 2
        if k > 0:
            inner(par, 3 if k < 2 else 2)
        receive_halo(k)
        if k == 0:
            lax.fori_loop(0, GX // 2, outer_weights, 0)
            for side in range(2):
                for held in (ohi, olo):
                    held[side, 1, 0, :TILE] = jnp.zeros((TILE, TILE), held.dtype)
                    held[side, GX // 2, 1, 3 * TILE :] = jnp.zeros((TILE, TILE), held.dtype)
        first, cross, square = outer(k, par)
        if k == 0:
            moments.append(first)
        if k < 2:
            moments += [cross, square]
            send_halo(k + 1)
        else:
            moments.append((2.0 * GAIN * amp) * cross - amp * moments[4])

    lane = lax.broadcasted_iota(jnp.int32, (RHS - 1, TILE), 1)
    packed = jnp.zeros((RHS - 1, TILE), F32)
    for i, part in enumerate(moments):
        total = jnp.sum(part, axis=1, keepdims=True)
        packed = jnp.where(lane == i, total[: RHS - 1], packed)
        packed = jnp.where(lane == i + len(moments), total[RHS - 1 : RHS], packed)
    mom[...] = packed
    gathered[me] = packed

    def mom_copy(k):
        peer = lax.rem(me + k, n)
        return pltpu.make_async_remote_copy(
            src_ref=mom,
            dst_ref=gathered.at[me],
            send_sem=mom_send.at[peer],
            recv_sem=mom_recv.at[me],
            device_id={"rows": peer},
            device_id_type=MESH,
        )

    def mom_start(k, carry):
        mom_copy(k).start()
        return carry

    lax.fori_loop(1, n, mom_start, 0)

    def mom_wait(k, carry):
        peer = lax.rem(me + k, n)
        pltpu.make_async_remote_copy(
            src_ref=mom,
            dst_ref=gathered.at[peer],
            send_sem=mom_send.at[peer],
            recv_sem=mom_recv.at[peer],
            device_id={"rows": peer},
            device_id_type=MESH,
        ).wait()
        return carry

    lax.fori_loop(1, n, mom_wait, 0)
    total = lax.fori_loop(0, n, lambda j, t: t + gathered[j], jnp.zeros((RHS - 1, TILE), F32))

    m = [
        jnp.concatenate([total[:, i : i + 1], total[:, i + 6 : i + 7]], axis=0)
        for i in range(6)
    ]
    a00, a01, a02 = (m[i + 1] + shift * m[i] for i in range(3))
    a11, a12 = (m[i + 1] + shift * m[i] for i in range(2, 4))
    a22 = m[5] + shift * m[4]
    l1 = a01 / a00
    l2 = a02 / a00
    b11 = a11 - l1 * a01
    b12 = a12 - l1 * a02
    b22 = a22 - l2 * a02
    g1 = m[1] - l1 * m[0]
    g2 = m[2] - l2 * m[0]
    fine1 = b11 > 1.0e-6 * a11
    safe1 = jnp.where(fine1, b11, 1.0)
    l3 = b12 / safe1
    d22 = b22 - l3 * b12
    fine2 = jnp.logical_and(fine1, d22 > 1.0e-6 * a22)
    c2 = jnp.where(fine2, (g2 - l3 * g1) / jnp.where(fine2, d22, 1.0), 0.0)
    c1 = jnp.where(fine1, (g1 - b12 * c2) / safe1, 0.0)
    c0 = (m[0] - a01 * c1 - a02 * c2) / a00
    values = (c0 * m[0] + c1 * m[1] + c2 * m[2]) / points
    flat = lax.broadcasted_iota(jnp.int32, (PAD, TILE), 1)
    sublane = lax.broadcasted_iota(jnp.int32, (PAD, TILE), 0)
    turned = jnp.sum(jnp.where(flat == sublane, values, 0.0), axis=0, keepdims=True)
    q_ref[...] = turned[:, :RHS]

    c0, c1, c2 = (jnp.broadcast_to(c, (PAD, TILE)) for c in (c0, c1, c2))
    for s in range(tiles):
        spot = cell[s]
        a, c = spot // GX, spot % GX
        found = c0 * vec[0, c, a] + c1 * vec[1, c, a] + c2 * vec[2, c, a]
        x_ref[:, s * TILE : (s + 1) * TILE] = found[:RHS]

    for k in range(3):
        for side in sends(k):
            @pl.when(has[side])
            def _(k=k, side=side):
                for copy in copies(k, side):
                    copy.wait_send()


def shards(n, offsets, tile_cell, probes, target, lengthscale, amplitude, noise):
    tiles = tile_cell.shape[0]
    rows = tiles // GX
    local = tiles * TILE
    wide = rows * TILE
    vmem = pl.BlockSpec(memory_space=pltpu.VMEM)
    solutions, quadratic = pl.pallas_call(
        functools.partial(kernel, n, rows, float(local * n)),
        out_shape=(
            jax.ShapeDtypeStruct((RHS, local), F32),
            jax.ShapeDtypeStruct((1, RHS), F32),
        ),
        in_specs=[pl.BlockSpec(memory_space=pltpu.HBM)] * 4
        + [pl.BlockSpec(memory_space=pltpu.SMEM)] * 3,
        out_specs=(vmem, vmem),
        scratch_shapes=[
            pltpu.SMEM((tiles,), jnp.int32),
            pltpu.VMEM((2, local), F32),
            pltpu.VMEM((RHS - 1, local), jnp.int32),
            pltpu.VMEM((1, local), F32),
            pltpu.VMEM((tiles, PAD, TILE), F32),
            pltpu.VMEM((3, GX, rows, PAD, TILE), F32),
            pltpu.VMEM((3, rows, GX, 1, TILE), F32),
            pltpu.VMEM((rows, GX, 2, TILE), F32),
            pltpu.VMEM((GX, rows, 2, TILE), F32),
            pltpu.VMEM((3, 2, GX, RHS - 1, TILE), F32),
            pltpu.VMEM((3, 2, GX, 1, TILE), F32),
            pltpu.VMEM((2, GX, 2, TILE), F32),
            pltpu.VMEM((2, GX + 2, 2 * PAD, wide), BF16),
            pltpu.VMEM((2, GX + 2, 2 * PAD, TILE), BF16),
            pltpu.VMEM((GX, 3, wide, wide), BF16),
            pltpu.VMEM((GX, 3, wide, wide), F8),
            pltpu.VMEM((2, GX // 2 + 2, 2, 4 * TILE, TILE), BF16),
            pltpu.VMEM((2, GX // 2 + 2, 2, 4 * TILE, TILE), F8),
            pltpu.VMEM((rows, 2, TILE, TILE), F32),
            pltpu.VMEM((rows, 2, TILE, TILE), F32),
            pltpu.VMEM((GX, PAD, wide), F32),
            pltpu.VMEM((RHS - 1, TILE), F32),
            pltpu.VMEM((n, RHS - 1, TILE), F32),
            pltpu.SMEM((tiles,), jnp.int32),
            pltpu.SemaphoreType.DMA((4,)),
            pltpu.SemaphoreType.DMA((3, 2, 3)),
            pltpu.SemaphoreType.DMA((3, 2, 3)),
            pltpu.SemaphoreType.DMA((n,)),
            pltpu.SemaphoreType.DMA((n,)),
        ],
        compiler_params=pltpu.CompilerParams(
            collective_id=0, has_side_effects=True, vmem_limit_bytes=52 * 1024 * 1024
        ),
        name="solve",
    )(
        *(
            pltpu.with_memory_space_constraint(x, pltpu.HBM)
            for x in (tile_cell, offsets, probes, target[None, :])
        ),
        lengthscale,
        amplitude,
        noise,
    )
    return solutions, quadratic.reshape(RHS)


def solution(mesh):
    return jax.shard_map(
        functools.partial(shards, mesh.shape["rows"]),
        mesh=mesh,
        in_specs=(
            P(None, "rows"),
            P("rows"),
            P(None, "rows"),
            P("rows"),
            P("hyp"),
            P("hyp"),
            P("hyp"),
        ),
        out_specs=(P("hyp", "rows"), P("hyp")),
        check_vma=False,
    )
```

```python
import functools

import jax
import jax.numpy as jnp
from jax import lax
from jax.experimental import pallas as pl
from jax.experimental.pallas import tpu as pltpu
from jax.sharding import PartitionSpec as P

TILE = 128
GX = 16
CUT = 8
RHS = 9
PAD = 16
FAR = 1.0e3
SCALE = 8.0
SNAP = 12.0 * SCALE
NUDGE = SCALE * 2.0**-21
GAIN = 4.0 / SCALE**5
MESH = pl.DeviceIdType.MESH
F32 = jnp.float32
BF16 = jnp.bfloat16
F8 = jnp.float8_e4m3fn


def snap(value):
    return (value + SNAP) - SNAP


def kernel(
    n, rows, points,
    cell_in, off_in, probes_in, target_in, length, amp_ref, noise_ref,
    x_ref, q_ref,
    cell, off, probes, target, raw, vec, snapped, outbox, inbox, hsnap,
    vx, vh, whi, wlo, ohi, olo, even, odd, acc, mom, gathered,
    powers, load_sem, halo_send, halo_recv, mom_send, mom_recv,
):
    tiles = rows * GX
    wide = rows * TILE
    me = lax.axis_index("rows")
    has = (me > 0, me < n - 1)

    barrier = pltpu.get_barrier_semaphore()

    def greet(k, carry):
        pl.semaphore_signal(
            barrier, inc=1, device_id={"rows": lax.rem(me + k, n)}, device_id_type=MESH
        )
        return carry

    loads = [
        pltpu.make_async_copy(source, held, load_sem.at[i])
        for i, (source, held) in enumerate(
            (
                (cell_in, cell), (off_in, off), (probes_in, probes), (target_in, target),
            )
        )
    ]
    for load in loads:
        load.start()
    lax.fori_loop(1, n, greet, 0)
    loads[0].wait()
    amp = amp_ref[0]
    shift = amp + noise_ref[0]

    for s in range(tiles):
        powers[s] = jnp.int32((1 << s) - ((1 << 32) if s == 31 else 0))
    words = [jnp.int32(0)] * (tiles - 1).bit_length()
    for s in range(tiles):
        bit = powers[cell[s]]
        words = [w | bit if (s >> b) & 1 else w for b, w in enumerate(words)]
    order = []
    for g in range(tiles):
        place_of = jnp.int32(0)
        for b, w in enumerate(words):
            one = lax.shift_right_logical(w, jnp.int32(g)) & 1
            place_of = place_of | lax.shift_left(one, jnp.int32(b))
        order.append(place_of)

    inverse = SCALE / jnp.full((1, TILE), length[0], F32)
    step = snap(inverse)

    def split(value):
        high = value.astype(BF16)
        return jnp.concatenate([high, (value - high.astype(F32)).astype(BF16)], axis=0)

    for edge in (0, GX + 1):
        for par in range(2):
            vx[par, edge] = jnp.zeros((2 * PAD, wide), BF16)
        for side in range(2):
            vh[side, edge] = jnp.zeros((2 * PAD, TILE), BF16)
    for held in (whi, wlo):
        held[0, 0] = jnp.zeros((wide, wide), held.dtype)
        held[GX - 1, 2] = jnp.zeros((wide, wide), held.dtype)

    for load in loads[1:]:
        load.wait()

    def pack(k, a, part, spot, value):
        for side, row in ((0, 0), (1, rows - 1)):
            if a == row:
                outbox[k, side, part, spot] = value[: RHS - 1]
                outbox[k, side, part, CUT, pl.ds(spot, 1)] = value[RHS - 1 : RHS]

    for g in range(tiles):
        at = slice(g * TILE, (g + 1) * TILE)
        raw[g] = jnp.concatenate(
            [
                2.0 * probes[:, at].astype(F32) - 1.0,
                target[:, at],
                off[:, at],
                jnp.zeros((PAD - RHS - 2, TILE), F32),
            ],
            axis=0,
        )
    kept = lax.broadcasted_iota(jnp.int32, (PAD, TILE), 0) < RHS
    for c in range(GX):
        for a in range(rows):
            value = raw[order[a * GX + c]]
            where = value[RHS : RHS + 2]
            value = jnp.where(kept, value, 0.0)
            vec[0, c, a] = value
            pack(0, a, c // CUT, c % CUT, value)
            for side, row in ((0, 0), (1, rows - 1)):
                if a == row:
                    for axis in range(2):
                        outbox[0, side, c // CUT, CUT + 1 + axis, c % CUT : c % CUT + 1] = where[axis : axis + 1]
            snapped[c, a] = snap(where * inverse)
            vx[0, c + 1, :, a * TILE : (a + 1) * TILE] = split(value)

    def copy(k, side, part):
        tiles_sent = CUT + (3 if k == 0 else 1)
        return pltpu.make_async_remote_copy(
            src_ref=outbox.at[k, side, part, 0:tiles_sent],
            dst_ref=inbox.at[k, 1 - side, part, 0:tiles_sent],
            send_sem=halo_send.at[k, side, part],
            recv_sem=halo_recv.at[k, 1 - side, part],
            device_id={"rows": me - 1 if side == 0 else me + 1},
            device_id_type=MESH,
        )

    def sends(k):
        return (0, 1) if k < 2 else (0,)

    def send_halo(k, part):
        for side in sends(k):
            @pl.when(has[side])
            def _(side=side):
                copy(k, side, part).start()

    def receive_halo(k):
        for side in sends(k):
            @pl.when(has[1 - side])
            def _(side=side):
                for part in range(2):
                    landed = inbox.at[k, 1 - side, part, 0 : CUT + (3 if k == 0 else 1)]
                    pltpu.make_async_remote_copy(
                        src_ref=landed,
                        dst_ref=landed,
                        send_sem=halo_send.at[k, side, part],
                        recv_sem=halo_recv.at[k, 1 - side, part],
                        device_id={"rows": me + 1 if side == 0 else me - 1},
                        device_id_type=MESH,
                    ).wait_recv()

            @pl.when(jnp.logical_not(has[1 - side]))
            def _(side=side):
                inbox[k, 1 - side] = jnp.zeros(inbox.shape[2:], F32)
                if k == 0:
                    for part in range(2):
                        inbox[0, 1 - side, part, CUT + 1 :] = jnp.full((2, CUT, TILE), FAR, F32)

            for c in range(GX):
                part, spot = c // CUT, c % CUT
                row = slice(spot, spot + 1)
                vh[1 - side, c + 1] = split(
                    jnp.concatenate(
                        [
                            inbox[k, 1 - side, part, spot],
                            inbox[k, 1 - side, part, CUT, row],
                            jnp.zeros((PAD - RHS, TILE), F32),
                        ],
                        axis=0,
                    )
                )
                if k == 0:
                    where = jnp.concatenate(
                        [inbox[0, 1 - side, part, CUT + 1 + axis, row] for axis in range(2)],
                        axis=0,
                    )
                    hsnap[1 - side, c] = snap(where * inverse)

    def spread(held, where):
        for axis in range(2):
            held[axis] = jnp.broadcast_to(where[axis : axis + 1], (TILE, TILE)).T

    def weights(held, where, down, right):
        tx = where[0:1] + (down * step + NUDGE)
        ty = where[1:2] + right * step
        high, low = [], []
        size = 64
        for part in range(TILE // size):
            at = slice(part * size, (part + 1) * size)
            dx = held[0, at, :] - tx
            dy = held[1, at, :] - ty
            square = dx * dx + dy * dy
            close = jnp.maximum(SCALE - square * lax.rsqrt(square), 0.0)
            twice = close * close
            w = twice * twice * (1.25 * SCALE - close)
            top = w.astype(BF16)
            high.append(top)
            low.append((w - top.astype(F32)).astype(F8))
        return jnp.concatenate(high, axis=0), jnp.concatenate(low, axis=0)

    def put(c, j, source, to, pair):
        down = slice(source * TILE, (source + 1) * TILE)
        right = slice(to * TILE, (to + 1) * TILE)
        whi[c, j, down, right] = pair[0]
        wlo[c, j, down, right] = pair[1]

    def column(c, held, fresh, more=True):
        if more:
            for a in range(rows):
                spread(fresh.at[a], snapped[c + 1, a])
        for a in range(rows):
            for b in range(a, rows):
                pair = weights(held.at[a], snapped[c, b], b - a, 0)
                put(c, 1, a, b, pair)
                if b > a:
                    put(c, 1, b, a, tuple(p.T for p in pair))
        if more:
            for a in range(rows):
                for b in range(rows):
                    pair = weights(held.at[a], snapped[c + 1, b], b - a, 1)
                    put(c + 1, 0, a, b, pair)
                    put(c, 2, b, a, tuple(p.T for p in pair))

    def two(i, carry):
        column(2 * i, even, odd)
        column(2 * i + 1, odd, even)
        return carry

    for a in range(rows):
        spread(even.at[a], snapped[0, a])
    half = GX // 2 - 1
    lax.fori_loop(0, half - 5, two, 0)
    pl.semaphore_wait(barrier, n - 1)
    send_halo(0, 0)
    send_halo(0, 1)
    lax.fori_loop(half - 5, half, two, 0)
    column(GX - 2, even, odd)
    column(GX - 1, odd, even, more=False)

    def apply(v, high, low):
        r = jnp.dot(v, high, preferred_element_type=F32)
        s = jnp.dot(v[:PAD], low, preferred_element_type=F32)
        return r[:PAD] + r[PAD:] + s

    def inner_run(par, count):
        def run(c, carry):
            v = [vx[par, c + j] for j in range(count)]
            if count < 3:
                v[1] = v[1] * BF16(0.5)
            high, low = (
                jnp.concatenate([held[c, j] for j in range(count)], axis=0)
                for held in (whi, wlo)
            )
            acc[c] = apply(jnp.concatenate(v, axis=1), high, low)
            return carry

        return run

    def inner(par, count):
        lax.fori_loop(0, GX, inner_run(par, count), 0, unroll=16)

    def outer_weights(p, carry):
        inner_run(0, 3)(2 * p, 0)
        inner_run(0, 3)(2 * p + 1, 0)
        for side in range(2):
            row = 0 if side == 0 else rows - 1
            down = 1 if side == 0 else -1
            for held in (ohi, olo):
                held[side, p + 1, 0, 3 * TILE :] = jnp.zeros((TILE, TILE), held.dtype)
                held[side, p + 1, 1, :TILE] = jnp.zeros((TILE, TILE), held.dtype)
            for t in range(2):
                c = 2 * p + t
                fresh = (even, odd)[side].at[t]
                spread(fresh, hsnap[side, c])
                for move in (-1, 0, 1):
                    spot = t + move
                    to, slot = p + 1 + spot // 2, spot % 2
                    source = t + 1 - 2 * (spot // 2)
                    near = jnp.clip(c + move, 0, GX - 1)
                    high, low = weights(fresh, snapped[near, row], down, move)
                    down_at = slice(source * TILE, (source + 1) * TILE)
                    ohi[side, to, slot, down_at] = high
                    olo[side, to, slot, down_at] = low
        return carry

    def outer(k, par):
        def run(p, carry):
            first, cross, square = carry
            edges = {}
            for side in (0, 1) if k < 2 else (1,):
                v = jnp.concatenate([vh[side, 2 * p + j] for j in range(4)], axis=1)
                high, low = (
                    jnp.concatenate([held[side, p + 1, t] for t in range(2)], axis=1)
                    for held in (ohi, olo)
                )
                edges[side] = apply(v, high, low)
            for t in range(2):
                c = 2 * p + t
                for a in range(rows):
                    total = acc[c, :, a * TILE : (a + 1) * TILE]
                    for side, row in ((0, 0), (1, rows - 1)):
                        if a == row and side in edges:
                            total = total + edges[side][:, t * TILE : (t + 1) * TILE]
                    now = vec[k, c, a]
                    if k < 2:
                        later = (GAIN * amp) * total - amp * now
                        if k == 0:
                            first = first + now * now
                        cross = cross + now * later
                        square = square + later * later
                        vec[k + 1, c, a] = later
                        pack(k + 1, a, c // CUT, c % CUT, later)
                        vx[1 - par, c + 1, :, a * TILE : (a + 1) * TILE] = split(later)
                    else:
                        cross = cross + now * total
            return first, cross, square

        return run

    blank = jnp.zeros((PAD, TILE), F32)
    pairs = GX // 2
    moments = []
    for k in range(3):
        par = k % 2
        if k > 0:
            inner(par, 3 if k < 2 else 2)
        receive_halo(k)
        run = outer(k, par)
        sums = (blank, blank, blank)
        if k == 0:
            for side in range(2):
                for held in (ohi, olo):
                    held[side, 1, 0, :TILE] = jnp.zeros((TILE, TILE), held.dtype)
                    held[side, pairs, 1, 3 * TILE :] = jnp.zeros((TILE, TILE), held.dtype)

            def both(p, carry):
                outer_weights(p, 0)
                return run(p - 2, carry)

            lax.fori_loop(0, 2, outer_weights, 0)
            sums = lax.fori_loop(2, pairs // 2 + 2, both, sums)
            send_halo(1, 0)
            sums = lax.fori_loop(pairs // 2 + 2, pairs, both, sums)
            sums = lax.fori_loop(pairs - 2, pairs, run, sums, unroll=2)
            send_halo(1, 1)
        elif k == 1:
            for part in range(2):
                half = pairs // 2
                sums = lax.fori_loop(part * half, (part + 1) * half, run, sums, unroll=half)
                send_halo(2, part)
        else:
            sums = lax.fori_loop(0, pairs, run, sums, unroll=pairs)
        first, cross, square = sums
        if k == 0:
            moments.append(first)
        if k < 2:
            moments += [cross, square]
        else:
            moments.append((2.0 * GAIN * amp) * cross - amp * moments[4])

    lane = lax.broadcasted_iota(jnp.int32, (RHS - 1, TILE), 1)
    packed = jnp.zeros((RHS - 1, TILE), F32)
    for i, part in enumerate(moments):
        total = jnp.sum(part, axis=1, keepdims=True)
        packed = jnp.where(lane == i, total[: RHS - 1], packed)
        packed = jnp.where(lane == i + len(moments), total[RHS - 1 : RHS], packed)
    mom[...] = packed
    gathered[me] = packed

    def mom_copy(k):
        peer = lax.rem(me + k, n)
        return pltpu.make_async_remote_copy(
            src_ref=mom,
            dst_ref=gathered.at[me],
            send_sem=mom_send.at[peer],
            recv_sem=mom_recv.at[me],
            device_id={"rows": peer},
            device_id_type=MESH,
        )

    def mom_start(k, carry):
        mom_copy(k).start()
        return carry

    lax.fori_loop(1, n, mom_start, 0)

    def mom_wait(k, carry):
        peer = lax.rem(me + k, n)
        pltpu.make_async_remote_copy(
            src_ref=mom,
            dst_ref=gathered.at[peer],
            send_sem=mom_send.at[peer],
            recv_sem=mom_recv.at[peer],
            device_id={"rows": peer},
            device_id_type=MESH,
        ).wait()
        return carry

    lax.fori_loop(1, n, mom_wait, 0)
    total = lax.fori_loop(0, n, lambda j, t: t + gathered[j], jnp.zeros((RHS - 1, TILE), F32))

    m = [
        jnp.concatenate([total[:, i : i + 1], total[:, i + 6 : i + 7]], axis=0)
        for i in range(6)
    ]
    a00, a01, a02 = (m[i + 1] + shift * m[i] for i in range(3))
    a11, a12 = (m[i + 1] + shift * m[i] for i in range(2, 4))
    a22 = m[5] + shift * m[4]
    l1 = a01 / a00
    l2 = a02 / a00
    b11 = a11 - l1 * a01
    b12 = a12 - l1 * a02
    b22 = a22 - l2 * a02
    g1 = m[1] - l1 * m[0]
    g2 = m[2] - l2 * m[0]
    fine1 = b11 > 1.0e-6 * a11
    safe1 = jnp.where(fine1, b11, 1.0)
    l3 = b12 / safe1
    d22 = b22 - l3 * b12
    fine2 = jnp.logical_and(fine1, d22 > 1.0e-6 * a22)
    c2 = jnp.where(fine2, (g2 - l3 * g1) / jnp.where(fine2, d22, 1.0), 0.0)
    c1 = jnp.where(fine1, (g1 - b12 * c2) / safe1, 0.0)
    c0 = (m[0] - a01 * c1 - a02 * c2) / a00
    values = (c0 * m[0] + c1 * m[1] + c2 * m[2]) / points
    flat = lax.broadcasted_iota(jnp.int32, (PAD, TILE), 1)
    sublane = lax.broadcasted_iota(jnp.int32, (PAD, TILE), 0)
    turned = jnp.sum(jnp.where(flat == sublane, values, 0.0), axis=0, keepdims=True)
    q_ref[...] = turned[:, :RHS]

    c0, c1, c2 = (jnp.broadcast_to(c, (PAD, TILE)) for c in (c0, c1, c2))
    for s in range(tiles):
        spot = cell[s]
        a, c = spot // GX, spot % GX
        found = c0 * vec[0, c, a] + c1 * vec[1, c, a] + c2 * vec[2, c, a]
        x_ref[:, s * TILE : (s + 1) * TILE] = found[:RHS]

    for k in range(3):
        for side in sends(k):
            @pl.when(has[side])
            def _(k=k, side=side):
                for part in range(2):
                    copy(k, side, part).wait_send()


def ship(x_in, q_in, x_out, q_out, sem):
    moves = [
        pltpu.make_async_copy(source, held, sem.at[i])
        for i, (source, held) in enumerate(((x_in, x_out), (q_in, q_out)))
    ]
    for move in moves:
        move.start()
    for move in moves:
        move.wait()


def shards(n, offsets, tile_cell, probes, target, lengthscale, amplitude, noise):
    tiles = tile_cell.shape[0]
    rows = tiles // GX
    local = tiles * TILE
    wide = rows * TILE
    vmem = pl.BlockSpec(memory_space=pltpu.VMEM)
    solutions, quadratic = pl.pallas_call(
        functools.partial(kernel, n, rows, float(local * n)),
        out_shape=(
            jax.ShapeDtypeStruct((RHS, local), F32),
            jax.ShapeDtypeStruct((1, RHS), F32),
        ),
        in_specs=[pl.BlockSpec(memory_space=pltpu.HBM)] * 4
        + [pl.BlockSpec(memory_space=pltpu.SMEM)] * 3,
        out_specs=(vmem, vmem),
        scratch_shapes=[
            pltpu.SMEM((tiles,), jnp.int32),
            pltpu.VMEM((2, local), F32),
            pltpu.VMEM((RHS - 1, local), jnp.int32),
            pltpu.VMEM((1, local), F32),
            pltpu.VMEM((tiles, PAD, TILE), F32),
            pltpu.VMEM((3, GX, rows, PAD, TILE), F32),
            pltpu.VMEM((GX, rows, 2, TILE), F32),
            pltpu.VMEM((3, 2, GX // CUT, CUT + 3, CUT, TILE), F32),
            pltpu.VMEM((3, 2, GX // CUT, CUT + 3, CUT, TILE), F32),
            pltpu.VMEM((2, GX, 2, TILE), F32),
            pltpu.VMEM((2, GX + 2, 2 * PAD, wide), BF16),
            pltpu.VMEM((2, GX + 2, 2 * PAD, TILE), BF16),
            pltpu.VMEM((GX, 3, wide, wide), BF16),
            pltpu.VMEM((GX, 3, wide, wide), F8),
            pltpu.VMEM((2, GX // 2 + 2, 2, 4 * TILE, TILE), BF16),
            pltpu.VMEM((2, GX // 2 + 2, 2, 4 * TILE, TILE), F8),
            pltpu.VMEM((rows, 2, TILE, TILE), F32),
            pltpu.VMEM((rows, 2, TILE, TILE), F32),
            pltpu.VMEM((GX, PAD, wide), F32),
            pltpu.VMEM((RHS - 1, TILE), F32),
            pltpu.VMEM((n, RHS - 1, TILE), F32),
            pltpu.SMEM((tiles,), jnp.int32),
            pltpu.SemaphoreType.DMA((4,)),
            pltpu.SemaphoreType.DMA((3, 2, 2)),
            pltpu.SemaphoreType.DMA((3, 2, 2)),
            pltpu.SemaphoreType.DMA((n,)),
            pltpu.SemaphoreType.DMA((n,)),
        ],
        compiler_params=pltpu.CompilerParams(
            collective_id=0, has_side_effects=True, vmem_limit_bytes=52 * 1024 * 1024
        ),
        name="solve",
    )(
        *(
            pltpu.with_memory_space_constraint(x, pltpu.HBM)
            for x in (tile_cell, offsets, probes, target[None, :])
        ),
        lengthscale,
        amplitude,
        noise,
    )
    hbm = pl.BlockSpec(memory_space=pltpu.HBM)
    solutions, quadratic = pl.pallas_call(
        ship,
        out_shape=(
            jax.ShapeDtypeStruct((RHS, local), F32),
            jax.ShapeDtypeStruct((1, RHS), F32),
        ),
        in_specs=[vmem, vmem],
        out_specs=(hbm, hbm),
        scratch_shapes=[pltpu.SemaphoreType.DMA((2,))],
        compiler_params=pltpu.CompilerParams(vmem_limit_bytes=4 * 1024 * 1024),
        name="ship",
    )(solutions, quadratic)
    return solutions, quadratic.reshape(RHS)


def solution(mesh):
    return jax.shard_map(
        functools.partial(shards, mesh.shape["rows"]),
        mesh=mesh,
        in_specs=(
            P(None, "rows"),
            P("rows"),
            P(None, "rows"),
            P("rows"),
            P("hyp"),
            P("hyp"),
            P("hyp"),
        ),
        out_specs=(P("hyp", "rows"), P("hyp")),
        check_vma=False,
    )
```

```python
import functools

import jax
import jax.numpy as jnp
from jax import lax
from jax.experimental import pallas as pl
from jax.experimental.pallas import tpu as pltpu
from jax.sharding import PartitionSpec as P

TILE = 128
GX = 16
CUT = 8
RHS = 9
PAD = 16
FAR = 1.0e3
SCALE = 8.0
SNAP = 12.0 * SCALE
NUDGE = SCALE * 2.0**-21
GAIN = 4.0 / SCALE**5
MESH = pl.DeviceIdType.MESH
F32 = jnp.float32
BF16 = jnp.bfloat16
F8 = jnp.float8_e4m3fn


def snap(value):
    return (value + SNAP) - SNAP


def kernel(
    n, rows, points,
    cell_in, off_in, probes_in, target_in, length, amp_ref, noise_ref,
    x_ref, q_ref,
    cell, off, probes, target, raw, vec, snapped, outbox, inbox, hsnap,
    vx, vh, whi, wlo, ohi, olo, even, odd, acc, reach, mom, gathered,
    powers, load_sem, halo_send, halo_recv, mom_send, mom_recv,
):
    tiles = rows * GX
    wide = rows * TILE
    me = lax.axis_index("rows")
    has = (me > 0, me < n - 1)

    barrier = pltpu.get_barrier_semaphore()

    def greet(k, carry):
        pl.semaphore_signal(
            barrier, inc=1, device_id={"rows": lax.rem(me + k, n)}, device_id_type=MESH
        )
        return carry

    loads = [
        pltpu.make_async_copy(source, held, load_sem.at[i])
        for i, (source, held) in enumerate(
            (
                (cell_in, cell), (off_in, off), (probes_in, probes), (target_in, target),
            )
        )
    ]
    for load in loads:
        load.start()
    for s in range(tiles):
        powers[s] = jnp.int32((1 << s) - ((1 << 32) if s == 31 else 0))
    lax.fori_loop(1, n, greet, 0)
    for load in loads:
        load.wait()
    amp = amp_ref[0]
    shift = amp + noise_ref[0]

    words = [jnp.int32(0)] * (tiles - 1).bit_length()
    for s in range(tiles):
        bit = powers[cell[s]]
        words = [w | bit if (s >> b) & 1 else w for b, w in enumerate(words)]
    order = []
    for g in range(tiles):
        place_of = jnp.int32(0)
        for b, w in enumerate(words):
            one = lax.shift_right_logical(w, jnp.int32(g)) & 1
            place_of = place_of | lax.shift_left(one, jnp.int32(b))
        order.append(place_of)

    inverse = SCALE / jnp.full((1, TILE), length[0], F32)
    step = snap(inverse)

    def split(value):
        high = value.astype(BF16)
        return jnp.concatenate([high, (value - high.astype(F32)).astype(BF16)], axis=0)

    for edge in (0, GX + 1):
        for par in range(2):
            vx[par, edge] = jnp.zeros((2 * PAD, wide), BF16)
        for side in range(2):
            vh[side, edge] = jnp.zeros((2 * PAD, TILE), BF16)
    for held in (whi, wlo):
        held[0, 0] = jnp.zeros((wide, wide), held.dtype)
        held[GX - 1, 2] = jnp.zeros((wide, wide), held.dtype)


    def pack(k, a, part, spot, value):
        for side, row in ((0, 0), (1, rows - 1)):
            if a == row:
                outbox[k, side, part, spot] = value[: RHS - 1]
                outbox[k, side, part, CUT, pl.ds(spot, 1)] = value[RHS - 1 : RHS]

    for g in range(tiles):
        at = slice(g * TILE, (g + 1) * TILE)
        raw[g] = jnp.concatenate(
            [
                2.0 * probes[:, at].astype(F32) - 1.0,
                target[:, at],
                off[:, at],
                jnp.zeros((PAD - RHS - 2, TILE), F32),
            ],
            axis=0,
        )
    kept = lax.broadcasted_iota(jnp.int32, (PAD, TILE), 0) < RHS
    for c in range(GX):
        for a in range(rows):
            value = raw[order[a * GX + c]]
            where = value[RHS : RHS + 2]
            value = jnp.where(kept, value, 0.0)
            vec[0, c, a] = value
            pack(0, a, c // CUT, c % CUT, value)
            for side, row in ((0, 0), (1, rows - 1)):
                if a == row:
                    for axis in range(2):
                        outbox[0, side, c // CUT, CUT + 1 + axis, c % CUT : c % CUT + 1] = where[axis : axis + 1]
            snapped[c, a] = snap(where * inverse)
            vx[0, c + 1, :, a * TILE : (a + 1) * TILE] = split(value)

    def copy(k, side, part):
        tiles_sent = CUT + (3 if k == 0 else 1)
        return pltpu.make_async_remote_copy(
            src_ref=outbox.at[k, side, part, 0:tiles_sent],
            dst_ref=inbox.at[k, 1 - side, part, 0:tiles_sent],
            send_sem=halo_send.at[k, side, part],
            recv_sem=halo_recv.at[k, 1 - side, part],
            device_id={"rows": me - 1 if side == 0 else me + 1},
            device_id_type=MESH,
        )

    def sends(k):
        return (0, 1) if k < 2 else (0,)

    def send_halo(k, part):
        for side in sends(k):
            @pl.when(has[side])
            def _(side=side):
                copy(k, side, part).start()

    def arrived(k, side, c):
        part, spot = c // CUT, c % CUT
        return jnp.concatenate(
            [
                inbox[k, side, part, spot],
                inbox[k, side, part, CUT, spot : spot + 1],
                jnp.zeros((PAD - RHS, TILE), F32),
            ],
            axis=0,
        )

    def receive_halo(k):
        for side in sends(k):
            @pl.when(has[1 - side])
            def _(side=side):
                for part in range(2):
                    landed = inbox.at[k, 1 - side, part, 0 : CUT + (3 if k == 0 else 1)]
                    pltpu.make_async_remote_copy(
                        src_ref=landed,
                        dst_ref=landed,
                        send_sem=halo_send.at[k, side, part],
                        recv_sem=halo_recv.at[k, 1 - side, part],
                        device_id={"rows": me + 1 if side == 0 else me - 1},
                        device_id_type=MESH,
                    ).wait_recv()

            @pl.when(jnp.logical_not(has[1 - side]))
            def _(side=side):
                inbox[k, 1 - side] = jnp.zeros(inbox.shape[2:], F32)
                if k == 0:
                    for part in range(2):
                        inbox[0, 1 - side, part, CUT + 1 :] = jnp.full((2, CUT, TILE), FAR, F32)

            if k == 2:
                return
            for c in range(GX):
                part, spot = c // CUT, c % CUT
                row = slice(spot, spot + 1)
                vh[1 - side, c + 1] = split(arrived(k, 1 - side, c))
                if k == 0:
                    where = jnp.concatenate(
                        [inbox[0, 1 - side, part, CUT + 1 + axis, row] for axis in range(2)],
                        axis=0,
                    )
                    hsnap[1 - side, c] = snap(where * inverse)

    def spread(held, where):
        for axis in range(2):
            held[axis] = jnp.broadcast_to(where[axis : axis + 1], (TILE, TILE)).T

    def weights(held, where, down, right):
        tx = where[0:1] + (down * step + NUDGE)
        ty = where[1:2] + right * step
        high, low = [], []
        size = 64
        for part in range(TILE // size):
            at = slice(part * size, (part + 1) * size)
            dx = held[0, at, :] - tx
            dy = held[1, at, :] - ty
            square = dx * dx + dy * dy
            close = jnp.maximum(SCALE - square * lax.rsqrt(square), 0.0)
            twice = close * close
            w = twice * twice * (1.25 * SCALE - close)
            top = w.astype(BF16)
            high.append(top)
            low.append((w - top.astype(F32)).astype(F8))
        return jnp.concatenate(high, axis=0), jnp.concatenate(low, axis=0)

    def put(c, j, source, to, pair):
        down = slice(source * TILE, (source + 1) * TILE)
        right = slice(to * TILE, (to + 1) * TILE)
        whi[c, j, down, right] = pair[0]
        wlo[c, j, down, right] = pair[1]

    def column(c, held, fresh, more=True):
        if more:
            for a in range(rows):
                spread(fresh.at[a], snapped[c + 1, a])
        for a in range(rows):
            for b in range(a, rows):
                pair = weights(held.at[a], snapped[c, b], b - a, 0)
                put(c, 1, a, b, pair)
                if b > a:
                    put(c, 1, b, a, tuple(p.T for p in pair))
        if more:
            for a in range(rows):
                for b in range(rows):
                    pair = weights(held.at[a], snapped[c + 1, b], b - a, 1)
                    put(c + 1, 0, a, b, pair)
                    put(c, 2, b, a, tuple(p.T for p in pair))

    def two(i, carry):
        column(2 * i, even, odd)
        column(2 * i + 1, odd, even)
        return carry

    for a in range(rows):
        spread(even.at[a], snapped[0, a])
    half = GX // 2 - 1
    lax.fori_loop(0, half - 6, two, 0)
    pl.semaphore_wait(barrier, n - 1)
    send_halo(0, 0)
    send_halo(0, 1)
    lax.fori_loop(half - 6, half, two, 0)
    column(GX - 2, even, odd)
    column(GX - 1, odd, even, more=False)

    def apply(v, high, low):
        r = jnp.dot(v, high, preferred_element_type=F32)
        s = jnp.dot(v[:PAD], low, preferred_element_type=F32)
        return r[:PAD] + r[PAD:] + s

    def inner_run(par, count):
        def run(c, carry):
            v = [vx[par, c + j] for j in range(count)]
            if count < 3:
                v[1] = v[1] * BF16(0.5)
            high, low = (
                jnp.concatenate([held[c, j] for j in range(count)], axis=0)
                for held in (whi, wlo)
            )
            acc[c] = apply(jnp.concatenate(v, axis=1), high, low)
            return carry

        return run

    def inner(par, count):
        lax.fori_loop(0, GX, inner_run(par, count), 0, unroll=16)

    def outer_weights(p, carry):
        inner_run(0, 3)(2 * p, 0)
        inner_run(0, 3)(2 * p + 1, 0)
        for side in range(2):
            row = 0 if side == 0 else rows - 1
            down = 1 if side == 0 else -1
            for held in (ohi, olo):
                held[side, p + 1, 0, 3 * TILE :] = jnp.zeros((TILE, TILE), held.dtype)
                held[side, p + 1, 1, :TILE] = jnp.zeros((TILE, TILE), held.dtype)
            for t in range(2):
                c = 2 * p + t
                fresh = (even, odd)[side].at[t]
                spread(fresh, hsnap[side, c])
                for move in (-1, 0, 1):
                    spot = t + move
                    to, slot = p + 1 + spot // 2, spot % 2
                    source = t + 1 - 2 * (spot // 2)
                    near = jnp.clip(c + move, 0, GX - 1)
                    high, low = weights(fresh, snapped[near, row], down, move)
                    down_at = slice(source * TILE, (source + 1) * TILE)
                    ohi[side, to, slot, down_at] = high
                    olo[side, to, slot, down_at] = low
        return carry

    def outer(k, par):
        def run(p, carry):
            first, cross, square = carry
            edges = {}
            for side in range(2):
                v = jnp.concatenate([vh[side, 2 * p + j] for j in range(4)], axis=1)
                high, low = (
                    jnp.concatenate([held[side, p + 1, t] for t in range(2)], axis=1)
                    for held in (ohi, olo)
                )
                edges[side] = apply(v, high, low)
            for t in range(2):
                c = 2 * p + t
                for a in range(rows):
                    total = acc[c, :, a * TILE : (a + 1) * TILE]
                    for side, row in ((0, 0), (1, rows - 1)):
                        if a == row:
                            total = total + edges[side][:, t * TILE : (t + 1) * TILE]
                    now = vec[k, c, a]
                    later = (GAIN * amp) * total - amp * now
                    if k == 0:
                        first = first + now * now
                    cross = cross + now * later
                    square = square + later * later
                    vec[k + 1, c, a] = later
                    pack(k + 1, a, c // CUT, c % CUT, later)
                    vx[1 - par, c + 1, :, a * TILE : (a + 1) * TILE] = split(later)
            return first, cross, square

        return run

    def across(v, held):
        return lax.dot_general(v, held, (((1,), (1,)), ((), ())), preferred_element_type=F32)

    def toward(p, carry):
        row = slice((rows - 1) * TILE, rows * TILE)
        v = jnp.concatenate([vx[0, 2 * p + t + 1, :, row] for t in range(2)], axis=1)
        high, low = (
            jnp.concatenate([held[1, p + 1, t] for t in range(2)], axis=1) for held in (ohi, olo)
        )
        r = across(v, high)
        reach[p] = r[:PAD] + r[PAD:] + across(v[:PAD], low)
        for t in range(2):
            for a in range(rows):
                c = 2 * p + t
                carry = carry + vec[2, c, a] * acc[c, :, a * TILE : (a + 1) * TILE]
        return carry

    blank = jnp.zeros((PAD, TILE), F32)
    pairs = GX // 2
    moments = []
    for k in range(3):
        par = k % 2
        if k > 0:
            inner(par, 3 if k < 2 else 2)
        if k == 2:
            cross = lax.fori_loop(0, pairs, toward, blank, unroll=pairs)
        receive_halo(k)
        run = outer(k, par)
        sums = (blank, blank, blank)
        if k == 0:
            for side in range(2):
                for held in (ohi, olo):
                    held[side, 1, 0, :TILE] = jnp.zeros((TILE, TILE), held.dtype)
                    held[side, pairs, 1, 3 * TILE :] = jnp.zeros((TILE, TILE), held.dtype)

            def both(p, carry):
                outer_weights(p, 0)
                return run(p - 2, carry)

            lax.fori_loop(0, 2, outer_weights, 0)
            sums = lax.fori_loop(2, pairs // 2 + 2, both, sums)
            send_halo(1, 0)
            sums = lax.fori_loop(pairs // 2 + 2, pairs, both, sums)
            sums = lax.fori_loop(pairs - 2, pairs, run, sums, unroll=2)
            send_halo(1, 1)
        elif k == 1:
            for part in range(2):
                half = pairs // 2
                sums = lax.fori_loop(part * half, (part + 1) * half, run, sums, unroll=half)
                send_halo(2, part)
        else:
            for c in range(GX):
                far = arrived(2, 1, c)
                for p in range(max(0, (c - 1) // 2), min(pairs, (c + 1) // 2 + 1)):
                    j = c - (2 * p - 1)
                    cross = cross + far * reach[p, :, j * TILE : (j + 1) * TILE]
        if k < 2:
            first, cross, square = sums
        if k == 0:
            moments.append(first)
        if k < 2:
            moments += [cross, square]
        else:
            moments.append((2.0 * GAIN * amp) * cross - amp * moments[4])

    lane = lax.broadcasted_iota(jnp.int32, (RHS - 1, TILE), 1)
    packed = jnp.zeros((RHS - 1, TILE), F32)
    for i, part in enumerate(moments):
        total = jnp.sum(part, axis=1, keepdims=True)
        packed = jnp.where(lane == i, total[: RHS - 1], packed)
        packed = jnp.where(lane == i + len(moments), total[RHS - 1 : RHS], packed)
    mom[...] = packed
    gathered[me] = packed

    def mom_copy(k):
        peer = lax.rem(me + k, n)
        return pltpu.make_async_remote_copy(
            src_ref=mom,
            dst_ref=gathered.at[me],
            send_sem=mom_send.at[peer],
            recv_sem=mom_recv.at[me],
            device_id={"rows": peer},
            device_id_type=MESH,
        )

    def mom_start(k, carry):
        mom_copy(k).start()
        return carry

    lax.fori_loop(1, n, mom_start, 0)

    def mom_wait(k, carry):
        peer = lax.rem(me + k, n)
        pltpu.make_async_remote_copy(
            src_ref=mom,
            dst_ref=gathered.at[peer],
            send_sem=mom_send.at[peer],
            recv_sem=mom_recv.at[peer],
            device_id={"rows": peer},
            device_id_type=MESH,
        ).wait()
        return carry

    lax.fori_loop(1, n, mom_wait, 0)
    total = lax.fori_loop(0, n, lambda j, t: t + gathered[j], jnp.zeros((RHS - 1, TILE), F32))

    m = [
        jnp.concatenate([total[:, i : i + 1], total[:, i + 6 : i + 7]], axis=0)
        for i in range(6)
    ]
    a00, a01, a02 = (m[i + 1] + shift * m[i] for i in range(3))
    a11, a12 = (m[i + 1] + shift * m[i] for i in range(2, 4))
    a22 = m[5] + shift * m[4]
    l1 = a01 / a00
    l2 = a02 / a00
    b11 = a11 - l1 * a01
    b12 = a12 - l1 * a02
    b22 = a22 - l2 * a02
    g1 = m[1] - l1 * m[0]
    g2 = m[2] - l2 * m[0]
    fine1 = b11 > 1.0e-6 * a11
    safe1 = jnp.where(fine1, b11, 1.0)
    l3 = b12 / safe1
    d22 = b22 - l3 * b12
    fine2 = jnp.logical_and(fine1, d22 > 1.0e-6 * a22)
    c2 = jnp.where(fine2, (g2 - l3 * g1) / jnp.where(fine2, d22, 1.0), 0.0)
    c1 = jnp.where(fine1, (g1 - b12 * c2) / safe1, 0.0)
    c0 = (m[0] - a01 * c1 - a02 * c2) / a00
    values = (c0 * m[0] + c1 * m[1] + c2 * m[2]) / points
    flat = lax.broadcasted_iota(jnp.int32, (PAD, TILE), 1)
    sublane = lax.broadcasted_iota(jnp.int32, (PAD, TILE), 0)
    turned = jnp.sum(jnp.where(flat == sublane, values, 0.0), axis=0, keepdims=True)
    q_ref[...] = turned[:, :RHS]

    c0, c1, c2 = (jnp.broadcast_to(c, (PAD, TILE)) for c in (c0, c1, c2))
    for s in range(tiles):
        spot = cell[s]
        a, c = spot // GX, spot % GX
        found = c0 * vec[0, c, a] + c1 * vec[1, c, a] + c2 * vec[2, c, a]
        x_ref[:, s * TILE : (s + 1) * TILE] = found[:RHS]

    for k in range(3):
        for side in sends(k):
            @pl.when(has[side])
            def _(k=k, side=side):
                for part in range(2):
                    copy(k, side, part).wait_send()


def ship(x_in, q_in, x_out, q_out, sem):
    moves = [
        pltpu.make_async_copy(source, held, sem.at[i])
        for i, (source, held) in enumerate(((x_in, x_out), (q_in, q_out)))
    ]
    for move in moves:
        move.start()
    for move in moves:
        move.wait()


def shards(n, offsets, tile_cell, probes, target, lengthscale, amplitude, noise):
    tiles = tile_cell.shape[0]
    rows = tiles // GX
    local = tiles * TILE
    wide = rows * TILE
    vmem = pl.BlockSpec(memory_space=pltpu.VMEM)
    solutions, quadratic = pl.pallas_call(
        functools.partial(kernel, n, rows, float(local * n)),
        out_shape=(
            jax.ShapeDtypeStruct((RHS, local), F32),
            jax.ShapeDtypeStruct((1, RHS), F32),
        ),
        in_specs=[pl.BlockSpec(memory_space=pltpu.HBM)] * 4
        + [pl.BlockSpec(memory_space=pltpu.SMEM)] * 3,
        out_specs=(vmem, vmem),
        scratch_shapes=[
            pltpu.SMEM((tiles,), jnp.int32),
            pltpu.VMEM((2, local), F32),
            pltpu.VMEM((RHS - 1, local), jnp.int32),
            pltpu.VMEM((1, local), F32),
            pltpu.VMEM((tiles, PAD, TILE), F32),
            pltpu.VMEM((3, GX, rows, PAD, TILE), F32),
            pltpu.VMEM((GX, rows, 2, TILE), F32),
            pltpu.VMEM((3, 2, GX // CUT, CUT + 3, CUT, TILE), F32),
            pltpu.VMEM((3, 2, GX // CUT, CUT + 3, CUT, TILE), F32),
            pltpu.VMEM((2, GX, 2, TILE), F32),
            pltpu.VMEM((2, GX + 2, 2 * PAD, wide), BF16),
            pltpu.VMEM((2, GX + 2, 2 * PAD, TILE), BF16),
            pltpu.VMEM((GX, 3, wide, wide), BF16),
            pltpu.VMEM((GX, 3, wide, wide), F8),
            pltpu.VMEM((2, GX // 2 + 2, 2, 4 * TILE, TILE), BF16),
            pltpu.VMEM((2, GX // 2 + 2, 2, 4 * TILE, TILE), F8),
            pltpu.VMEM((rows, 2, TILE, TILE), F32),
            pltpu.VMEM((rows, 2, TILE, TILE), F32),
            pltpu.VMEM((GX, PAD, wide), F32),
            pltpu.VMEM((GX // 2, PAD, 4 * TILE), F32),
            pltpu.VMEM((RHS - 1, TILE), F32),
            pltpu.VMEM((n, RHS - 1, TILE), F32),
            pltpu.SMEM((tiles,), jnp.int32),
            pltpu.SemaphoreType.DMA((4,)),
            pltpu.SemaphoreType.DMA((3, 2, 2)),
            pltpu.SemaphoreType.DMA((3, 2, 2)),
            pltpu.SemaphoreType.DMA((n,)),
            pltpu.SemaphoreType.DMA((n,)),
        ],
        compiler_params=pltpu.CompilerParams(
            collective_id=0, has_side_effects=True, vmem_limit_bytes=52 * 1024 * 1024
        ),
        name="solve",
    )(
        *(
            pltpu.with_memory_space_constraint(x, pltpu.HBM)
            for x in (tile_cell, offsets, probes, target[None, :])
        ),
        lengthscale,
        amplitude,
        noise,
    )
    hbm = pl.BlockSpec(memory_space=pltpu.HBM)
    solutions, quadratic = pl.pallas_call(
        ship,
        out_shape=(
            jax.ShapeDtypeStruct((RHS, local), F32),
            jax.ShapeDtypeStruct((1, RHS), F32),
        ),
        in_specs=[vmem, vmem],
        out_specs=(hbm, hbm),
        scratch_shapes=[pltpu.SemaphoreType.DMA((2,))],
        compiler_params=pltpu.CompilerParams(vmem_limit_bytes=4 * 1024 * 1024),
        name="ship",
    )(solutions, quadratic)
    return solutions, quadratic.reshape(RHS)


def solution(mesh):
    return jax.shard_map(
        functools.partial(shards, mesh.shape["rows"]),
        mesh=mesh,
        in_specs=(
            P(None, "rows"),
            P("rows"),
            P(None, "rows"),
            P("rows"),
            P("hyp"),
            P("hyp"),
            P("hyp"),
        ),
        out_specs=(P("hyp", "rows"), P("hyp")),
        check_vma=False,
    )
```

```python
import functools

import jax
import jax.numpy as jnp
from jax import lax
from jax.experimental import pallas as pl
from jax.experimental.pallas import tpu as pltpu
from jax.sharding import PartitionSpec as P

TILE = 128
GX = 16
CUT = 8
RHS = 9
PAD = 16
FAR = 1.0e3
SCALE = 8.0
SNAP = 12.0 * SCALE
NUDGE = SCALE * 2.0**-21
GAIN = 4.0 / SCALE**5
MESH = pl.DeviceIdType.MESH
F32 = jnp.float32
BF16 = jnp.bfloat16
F8 = jnp.float8_e4m3fn


def snap(value):
    return (value + SNAP) - SNAP


def kernel(
    n, rows, points,
    cell_in, off_in, probes_in, target_in, length, amp_ref, noise_ref,
    x_ref, q_ref,
    cell, off, probes, target, raw, vec, snapped, outbox, inbox, hsnap,
    vx, vh, whi, wlo, ohi, olo, even, odd, acc, reach, mom, gathered,
    powers, load_sem, halo_send, halo_recv, mom_send, mom_recv,
):
    tiles = rows * GX
    wide = rows * TILE
    me = lax.axis_index("rows")
    has = (me > 0, me < n - 1)

    barrier = pltpu.get_barrier_semaphore()

    def greet(k, carry):
        pl.semaphore_signal(
            barrier, inc=1, device_id={"rows": lax.rem(me + k, n)}, device_id_type=MESH
        )
        return carry

    loads = [
        pltpu.make_async_copy(source, held, load_sem.at[i])
        for i, (source, held) in enumerate(
            (
                (cell_in, cell), (off_in, off), (probes_in, probes), (target_in, target),
            )
        )
    ]
    for load in loads:
        load.start()
    for s in range(tiles):
        powers[s] = jnp.int32((1 << s) - ((1 << 32) if s == 31 else 0))
    lax.fori_loop(1, n, greet, 0)
    for load in loads:
        load.wait()
    amp = amp_ref[0]
    shift = amp + noise_ref[0]

    words = [jnp.int32(0)] * (tiles - 1).bit_length()
    for s in range(tiles):
        bit = powers[cell[s]]
        words = [w | bit if (s >> b) & 1 else w for b, w in enumerate(words)]
    order = []
    for g in range(tiles):
        place_of = jnp.int32(0)
        for b, w in enumerate(words):
            one = lax.shift_right_logical(w, jnp.int32(g)) & 1
            place_of = place_of | lax.shift_left(one, jnp.int32(b))
        order.append(place_of)

    inverse = SCALE / jnp.full((1, TILE), length[0], F32)
    step = snap(inverse)

    def split(value):
        high = value.astype(BF16)
        return jnp.concatenate([high, (value - high.astype(F32)).astype(BF16)], axis=0)

    for edge in (0, GX + 1):
        for par in range(2):
            vx[par, edge] = jnp.zeros((2 * PAD, wide), BF16)
        for side in range(2):
            vh[side, edge] = jnp.zeros((2 * PAD, TILE), BF16)
    for held in (whi, wlo):
        held[0, 0] = jnp.zeros((wide, wide), held.dtype)
        held[GX - 1, 2] = jnp.zeros((wide, wide), held.dtype)


    def pack(k, a, part, spot, value):
        for side, row in ((0, 0), (1, rows - 1)):
            if a == row:
                outbox[k, side, part, spot] = value[: RHS - 1]
                outbox[k, side, part, CUT, pl.ds(spot, 1)] = value[RHS - 1 : RHS]

    for g in range(tiles):
        at = slice(g * TILE, (g + 1) * TILE)
        raw[g] = jnp.concatenate(
            [
                2.0 * probes[:, at].astype(F32) - 1.0,
                target[:, at],
                off[:, at],
                jnp.zeros((PAD - RHS - 2, TILE), F32),
            ],
            axis=0,
        )
    kept = lax.broadcasted_iota(jnp.int32, (PAD, TILE), 0) < RHS
    for c in range(GX):
        for a in range(rows):
            value = raw[order[a * GX + c]]
            where = value[RHS : RHS + 2]
            value = jnp.where(kept, value, 0.0)
            vec[0, c, a] = value
            pack(0, a, c // CUT, c % CUT, value)
            for side, row in ((0, 0), (1, rows - 1)):
                if a == row:
                    for axis in range(2):
                        outbox[0, side, c // CUT, CUT + 1 + axis, c % CUT : c % CUT + 1] = where[axis : axis + 1]
            snapped[c, a] = snap(where * inverse)
            vx[0, c + 1, :, a * TILE : (a + 1) * TILE] = split(value)

    def copy(k, side, part):
        tiles_sent = CUT + (3 if k == 0 else 1)
        return pltpu.make_async_remote_copy(
            src_ref=outbox.at[k, side, part, 0:tiles_sent],
            dst_ref=inbox.at[k, 1 - side, part, 0:tiles_sent],
            send_sem=halo_send.at[k, side, part],
            recv_sem=halo_recv.at[k, 1 - side, part],
            device_id={"rows": me - 1 if side == 0 else me + 1},
            device_id_type=MESH,
        )

    def sends(k):
        return (0, 1) if k < 2 else (0,)

    def send_halo(k, part):
        for side in sends(k):
            @pl.when(has[side])
            def _(side=side):
                copy(k, side, part).start()

    def arrived(k, side, c):
        part, spot = c // CUT, c % CUT
        return jnp.concatenate(
            [
                inbox[k, side, part, spot],
                inbox[k, side, part, CUT, spot : spot + 1],
                jnp.zeros((PAD - RHS, TILE), F32),
            ],
            axis=0,
        )

    def receive_halo(k):
        for side in sends(k):
            @pl.when(has[1 - side])
            def _(side=side):
                for part in range(2):
                    landed = inbox.at[k, 1 - side, part, 0 : CUT + (3 if k == 0 else 1)]
                    pltpu.make_async_remote_copy(
                        src_ref=landed,
                        dst_ref=landed,
                        send_sem=halo_send.at[k, side, part],
                        recv_sem=halo_recv.at[k, 1 - side, part],
                        device_id={"rows": me + 1 if side == 0 else me - 1},
                        device_id_type=MESH,
                    ).wait_recv()

            @pl.when(jnp.logical_not(has[1 - side]))
            def _(side=side):
                inbox[k, 1 - side] = jnp.zeros(inbox.shape[2:], F32)
                if k == 0:
                    for part in range(2):
                        inbox[0, 1 - side, part, CUT + 1 :] = jnp.full((2, CUT, TILE), FAR, F32)

            if k == 2:
                return
            for c in range(GX):
                part, spot = c // CUT, c % CUT
                row = slice(spot, spot + 1)
                vh[1 - side, c + 1] = split(arrived(k, 1 - side, c))
                if k == 0:
                    where = jnp.concatenate(
                        [inbox[0, 1 - side, part, CUT + 1 + axis, row] for axis in range(2)],
                        axis=0,
                    )
                    hsnap[1 - side, c] = snap(where * inverse)

    def spread(held, where):
        for axis in range(2):
            held[axis] = jnp.broadcast_to(where[axis : axis + 1], (TILE, TILE)).T

    def weights(held, where, down, right):
        tx = where[0:1] + (down * step + NUDGE)
        ty = where[1:2] + right * step
        high, low = [], []
        size = 64
        for part in range(TILE // size):
            at = slice(part * size, (part + 1) * size)
            dx = held[0, at, :] - tx
            dy = held[1, at, :] - ty
            square = dx * dx + dy * dy
            close = jnp.maximum(SCALE - square * lax.rsqrt(square), 0.0)
            twice = close * close
            w = twice * twice * (1.25 * SCALE - close)
            top = w.astype(BF16)
            high.append(top)
            low.append((w - top.astype(F32)).astype(F8))
        return jnp.concatenate(high, axis=0), jnp.concatenate(low, axis=0)

    def put(c, j, source, to, pair):
        down = slice(source * TILE, (source + 1) * TILE)
        right = slice(to * TILE, (to + 1) * TILE)
        whi[c, j, down, right] = pair[0]
        wlo[c, j, down, right] = pair[1]

    def column(c, held, fresh, more=True):
        if more:
            for a in range(rows):
                spread(fresh.at[a], snapped[c + 1, a])
        for a in range(rows):
            for b in range(a, rows):
                pair = weights(held.at[a], snapped[c, b], b - a, 0)
                put(c, 1, a, b, pair)
                if b > a:
                    put(c, 1, b, a, tuple(p.T for p in pair))
        if more:
            for a in range(rows):
                for b in range(rows):
                    pair = weights(held.at[a], snapped[c + 1, b], b - a, 1)
                    put(c + 1, 0, a, b, pair)
                    put(c, 2, b, a, tuple(p.T for p in pair))

    def two(i, carry):
        column(2 * i, even, odd)
        column(2 * i + 1, odd, even)
        return carry

    for a in range(rows):
        spread(even.at[a], snapped[0, a])
    half = GX // 2 - 1
    lax.fori_loop(0, half - 6, two, 0)
    pl.semaphore_wait(barrier, n - 1)
    send_halo(0, 0)
    send_halo(0, 1)
    lax.fori_loop(half - 6, half, two, 0)
    column(GX - 2, even, odd)
    column(GX - 1, odd, even, more=False)

    def apply(v, high, low):
        r = jnp.dot(v, high, preferred_element_type=F32)
        s = jnp.dot(v[:PAD], low, preferred_element_type=F32)
        return r[:PAD] + r[PAD:] + s

    def inner_run(par, count):
        def run(c, carry):
            v = [vx[par, c + j] for j in range(count)]
            if count < 3:
                v[1] = v[1] * BF16(0.5)
            high, low = (
                jnp.concatenate([held[c, j] for j in range(count)], axis=0)
                for held in (whi, wlo)
            )
            acc[c] = apply(jnp.concatenate(v, axis=1), high, low)
            return carry

        return run

    def inner(par, count):
        lax.fori_loop(0, GX, inner_run(par, count), 0, unroll=16)

    def outer_weights(p, carry):
        for side in range(2):
            inner_run(0, 3)(2 * p + side, 0)
            row = 0 if side == 0 else rows - 1
            down = 1 if side == 0 else -1
            for held in (ohi, olo):
                held[side, p + 1, 0, 3 * TILE :] = jnp.zeros((TILE, TILE), held.dtype)
                held[side, p + 1, 1, :TILE] = jnp.zeros((TILE, TILE), held.dtype)
            for t in range(2):
                c = 2 * p + t
                fresh = (even, odd)[side].at[t]
                spread(fresh, hsnap[side, c])
                for move in (-1, 0, 1):
                    spot = t + move
                    to, slot = p + 1 + spot // 2, spot % 2
                    source = t + 1 - 2 * (spot // 2)
                    near = jnp.clip(c + move, 0, GX - 1)
                    high, low = weights(fresh, snapped[near, row], down, move)
                    down_at = slice(source * TILE, (source + 1) * TILE)
                    ohi[side, to, slot, down_at] = high
                    olo[side, to, slot, down_at] = low
        return carry

    def outer(k, par):
        def run(p, carry):
            first, cross, square = carry
            edges = {}
            for side in range(2):
                edges[side] = jnp.concatenate(
                    [
                        apply(
                            jnp.concatenate([vh[side, 2 * p + t + j] for j in range(3)], axis=1),
                            *(
                                held[side, p + 1, t, t * TILE : (t + 3) * TILE]
                                for held in (ohi, olo)
                            ),
                        )
                        for t in range(2)
                    ],
                    axis=1,
                )
            for t in range(2):
                c = 2 * p + t
                for a in range(rows):
                    total = acc[c, :, a * TILE : (a + 1) * TILE]
                    for side, row in ((0, 0), (1, rows - 1)):
                        if a == row:
                            total = total + edges[side][:, t * TILE : (t + 1) * TILE]
                    now = vec[k, c, a]
                    later = (GAIN * amp) * total - amp * now
                    if k == 0:
                        first = first + now * now
                    cross = cross + now * later
                    square = square + later * later
                    vec[k + 1, c, a] = later
                    pack(k + 1, a, c // CUT, c % CUT, later)
                    vx[1 - par, c + 1, :, a * TILE : (a + 1) * TILE] = split(later)
            return first, cross, square

        return run

    def across(v, held):
        return lax.dot_general(v, held, (((1,), (1,)), ((), ())), preferred_element_type=F32)

    def toward(p, carry):
        row = slice((rows - 1) * TILE, rows * TILE)
        v = jnp.concatenate([vx[0, 2 * p + t + 1, :, row] for t in range(2)], axis=1)
        high, low = (
            jnp.concatenate([held[1, p + 1, t] for t in range(2)], axis=1) for held in (ohi, olo)
        )
        r = across(v, high)
        reach[p] = r[:PAD] + r[PAD:] + across(v[:PAD], low)
        for t in range(2):
            for a in range(rows):
                c = 2 * p + t
                carry = carry + vec[2, c, a] * acc[c, :, a * TILE : (a + 1) * TILE]
        return carry

    blank = jnp.zeros((PAD, TILE), F32)
    pairs = GX // 2
    moments = []
    for k in range(3):
        par = k % 2
        if k > 0:
            inner(par, 3 if k < 2 else 2)
        if k == 2:
            cross = lax.fori_loop(0, pairs, toward, blank, unroll=pairs)
        receive_halo(k)
        run = outer(k, par)
        sums = (blank, blank, blank)
        if k == 0:
            for side in range(2):
                for held in (ohi, olo):
                    held[side, 1, 0, :TILE] = jnp.zeros((TILE, TILE), held.dtype)
                    held[side, pairs, 1, 3 * TILE :] = jnp.zeros((TILE, TILE), held.dtype)

            def both(p, carry):
                outer_weights(p, 0)
                return run(p - 2, carry)

            lax.fori_loop(0, 2, outer_weights, 0)
            sums = lax.fori_loop(2, pairs // 2 + 2, both, sums)
            send_halo(1, 0)
            sums = lax.fori_loop(pairs // 2 + 2, pairs, both, sums)
            sums = lax.fori_loop(pairs - 2, pairs, run, sums, unroll=2)
            send_halo(1, 1)
        elif k == 1:
            for part in range(2):
                half = pairs // 2
                sums = lax.fori_loop(part * half, (part + 1) * half, run, sums, unroll=half)
                send_halo(2, part)
        else:
            for c in range(GX):
                far = arrived(2, 1, c)
                for p in range(max(0, (c - 1) // 2), min(pairs, (c + 1) // 2 + 1)):
                    j = c - (2 * p - 1)
                    cross = cross + far * reach[p, :, j * TILE : (j + 1) * TILE]
        if k < 2:
            first, cross, square = sums
        if k == 0:
            moments.append(first)
        if k < 2:
            moments += [cross, square]
        else:
            moments.append((2.0 * GAIN * amp) * cross - amp * moments[4])

    lane = lax.broadcasted_iota(jnp.int32, (RHS - 1, TILE), 1)
    packed = jnp.zeros((RHS - 1, TILE), F32)
    for i, part in enumerate(moments):
        total = jnp.sum(part, axis=1, keepdims=True)
        packed = jnp.where(lane == i, total[: RHS - 1], packed)
        packed = jnp.where(lane == i + len(moments), total[RHS - 1 : RHS], packed)
    mom[...] = packed
    gathered[me] = packed

    def mom_copy(k):
        peer = lax.rem(me + k, n)
        return pltpu.make_async_remote_copy(
            src_ref=mom,
            dst_ref=gathered.at[me],
            send_sem=mom_send.at[peer],
            recv_sem=mom_recv.at[me],
            device_id={"rows": peer},
            device_id_type=MESH,
        )

    def mom_start(k, carry):
        mom_copy(k).start()
        return carry

    lax.fori_loop(1, n, mom_start, 0)

    def mom_wait(k, carry):
        peer = lax.rem(me + k, n)
        pltpu.make_async_remote_copy(
            src_ref=mom,
            dst_ref=gathered.at[peer],
            send_sem=mom_send.at[peer],
            recv_sem=mom_recv.at[peer],
            device_id={"rows": peer},
            device_id_type=MESH,
        ).wait()
        return carry

    lax.fori_loop(1, n, mom_wait, 0)
    total = lax.fori_loop(0, n, lambda j, t: t + gathered[j], jnp.zeros((RHS - 1, TILE), F32))

    m = [
        jnp.concatenate([total[:, i : i + 1], total[:, i + 6 : i + 7]], axis=0)
        for i in range(6)
    ]
    a00, a01, a02 = (m[i + 1] + shift * m[i] for i in range(3))
    a11, a12 = (m[i + 1] + shift * m[i] for i in range(2, 4))
    a22 = m[5] + shift * m[4]
    l1 = a01 / a00
    l2 = a02 / a00
    b11 = a11 - l1 * a01
    b12 = a12 - l1 * a02
    b22 = a22 - l2 * a02
    g1 = m[1] - l1 * m[0]
    g2 = m[2] - l2 * m[0]
    fine1 = b11 > 1.0e-6 * a11
    safe1 = jnp.where(fine1, b11, 1.0)
    l3 = b12 / safe1
    d22 = b22 - l3 * b12
    fine2 = jnp.logical_and(fine1, d22 > 1.0e-6 * a22)
    c2 = jnp.where(fine2, (g2 - l3 * g1) / jnp.where(fine2, d22, 1.0), 0.0)
    c1 = jnp.where(fine1, (g1 - b12 * c2) / safe1, 0.0)
    c0 = (m[0] - a01 * c1 - a02 * c2) / a00
    values = (c0 * m[0] + c1 * m[1] + c2 * m[2]) / points
    flat = lax.broadcasted_iota(jnp.int32, (PAD, TILE), 1)
    sublane = lax.broadcasted_iota(jnp.int32, (PAD, TILE), 0)
    turned = jnp.sum(jnp.where(flat == sublane, values, 0.0), axis=0, keepdims=True)
    q_ref[...] = turned[:, :RHS]

    c0, c1, c2 = (jnp.broadcast_to(c, (PAD, TILE)) for c in (c0, c1, c2))
    for s in range(tiles):
        spot = cell[s]
        a, c = spot // GX, spot % GX
        found = c0 * vec[0, c, a] + c1 * vec[1, c, a] + c2 * vec[2, c, a]
        x_ref[:, s * TILE : (s + 1) * TILE] = found[:RHS]

    for k in range(3):
        for side in sends(k):
            @pl.when(has[side])
            def _(k=k, side=side):
                for part in range(2):
                    copy(k, side, part).wait_send()


def ship(x_in, q_in, x_out, q_out, sem):
    moves = [
        pltpu.make_async_copy(source, held, sem.at[i])
        for i, (source, held) in enumerate(((x_in, x_out), (q_in, q_out)))
    ]
    for move in moves:
        move.start()
    for move in moves:
        move.wait()


def shards(n, offsets, tile_cell, probes, target, lengthscale, amplitude, noise):
    tiles = tile_cell.shape[0]
    rows = tiles // GX
    local = tiles * TILE
    wide = rows * TILE
    vmem = pl.BlockSpec(memory_space=pltpu.VMEM)
    solutions, quadratic = pl.pallas_call(
        functools.partial(kernel, n, rows, float(local * n)),
        out_shape=(
            jax.ShapeDtypeStruct((RHS, local), F32),
            jax.ShapeDtypeStruct((1, RHS), F32),
        ),
        in_specs=[pl.BlockSpec(memory_space=pltpu.HBM)] * 4
        + [pl.BlockSpec(memory_space=pltpu.SMEM)] * 3,
        out_specs=(vmem, vmem),
        scratch_shapes=[
            pltpu.SMEM((tiles,), jnp.int32),
            pltpu.VMEM((2, local), F32),
            pltpu.VMEM((RHS - 1, local), jnp.int32),
            pltpu.VMEM((1, local), F32),
            pltpu.VMEM((tiles, PAD, TILE), F32),
            pltpu.VMEM((3, GX, rows, PAD, TILE), F32),
            pltpu.VMEM((GX, rows, 2, TILE), F32),
            pltpu.VMEM((3, 2, GX // CUT, CUT + 3, CUT, TILE), F32),
            pltpu.VMEM((3, 2, GX // CUT, CUT + 3, CUT, TILE), F32),
            pltpu.VMEM((2, GX, 2, TILE), F32),
            pltpu.VMEM((2, GX + 2, 2 * PAD, wide), BF16),
            pltpu.VMEM((2, GX + 2, 2 * PAD, TILE), BF16),
            pltpu.VMEM((GX, 3, wide, wide), BF16),
            pltpu.VMEM((GX, 3, wide, wide), F8),
            pltpu.VMEM((2, GX // 2 + 2, 2, 4 * TILE, TILE), BF16),
            pltpu.VMEM((2, GX // 2 + 2, 2, 4 * TILE, TILE), F8),
            pltpu.VMEM((rows, 2, TILE, TILE), F32),
            pltpu.VMEM((rows, 2, TILE, TILE), F32),
            pltpu.VMEM((GX, PAD, wide), F32),
            pltpu.VMEM((GX // 2, PAD, 4 * TILE), F32),
            pltpu.VMEM((RHS - 1, TILE), F32),
            pltpu.VMEM((n, RHS - 1, TILE), F32),
            pltpu.SMEM((tiles,), jnp.int32),
            pltpu.SemaphoreType.DMA((4,)),
            pltpu.SemaphoreType.DMA((3, 2, 2)),
            pltpu.SemaphoreType.DMA((3, 2, 2)),
            pltpu.SemaphoreType.DMA((n,)),
            pltpu.SemaphoreType.DMA((n,)),
        ],
        compiler_params=pltpu.CompilerParams(
            collective_id=0, has_side_effects=True, vmem_limit_bytes=52 * 1024 * 1024
        ),
        name="solve",
    )(
        *(
            pltpu.with_memory_space_constraint(x, pltpu.HBM)
            for x in (tile_cell, offsets, probes, target[None, :])
        ),
        lengthscale,
        amplitude,
        noise,
    )
    hbm = pl.BlockSpec(memory_space=pltpu.HBM)
    solutions, quadratic = pl.pallas_call(
        ship,
        out_shape=(
            jax.ShapeDtypeStruct((RHS, local), F32),
            jax.ShapeDtypeStruct((1, RHS), F32),
        ),
        in_specs=[vmem, vmem],
        out_specs=(hbm, hbm),
        scratch_shapes=[pltpu.SemaphoreType.DMA((2,))],
        compiler_params=pltpu.CompilerParams(vmem_limit_bytes=4 * 1024 * 1024),
        name="ship",
    )(solutions, quadratic)
    return solutions, quadratic.reshape(RHS)


def solution(mesh):
    return jax.shard_map(
        functools.partial(shards, mesh.shape["rows"]),
        mesh=mesh,
        in_specs=(
            P(None, "rows"),
            P("rows"),
            P(None, "rows"),
            P("rows"),
            P("hyp"),
            P("hyp"),
            P("hyp"),
        ),
        out_specs=(P("hyp", "rows"), P("hyp")),
        check_vma=False,
    )
```
